512 devices in a mesh: groups: 2 (over y), ffn: 32 (over z), hidden: 8 (over x, core).
Axes of the slice: x: 4, y: 2, z: 32, core: 2. Of those that a mesh axis runs over, the one named last changes fastest.
The devices are a block of a 4x8x32 slice.
Arguments:
- residual_in: bfloat16 [1024, 8192], P(('groups', 'ffn'), 'hidden'), parts along dimension 0, may hold values from -10 to 10
- queries: bfloat16 [1024, 8192], P(('groups', 'hidden'), 'ffn'), parts along dimension 0, may hold values from -100 to 100
- new_keys: bfloat16 [1024, 1024], P(('groups', 'hidden'), 'ffn'), parts along dimension 0, may hold values from -6 to 6
- new_values: bfloat16 [1024, 1024], P(('groups', 'hidden'), 'ffn'), parts along dimension 0, may hold values from -24 to 24
- key_cache: bfloat16 [64, 2048, 1024], P(('groups', 'hidden'), 'ffn'), parts along dimension 0, may hold values from -6 to 6
- value_cache: bfloat16 [64, 2048, 1024], P(('groups', 'hidden'), 'ffn'), parts along dimension 0, may hold values from -24 to 24
- cache_lengths: int32 [64], P(('groups', 'hidden')), parts along dimension 0, may hold values from 1 to 2048, as said below
- norm_gain: bfloat16 [8192], P('hidden'), may hold values from 0.099609375 to 1.8984375
- out_weight: bfloat16 [8192, 8192], P('ffn', 'hidden'), may hold values from -0.25 to 0.25
- gate_weight: bfloat16 [8192, 14336], P('hidden', 'ffn'), may hold values from -0.125 to 0.125
- up_weight: bfloat16 [8192, 14336], P('hidden', 'ffn'), may hold values from -0.125 to 0.125
- down_weight: bfloat16 [14336, 8192], P('ffn', 'hidden'), may hold values from -0.09375 to 0.09375
Outputs:
- block_out: bfloat16 [1024, 8192], P(('groups', 'ffn'), 'hidden'), parts along dimension 0
The draws below stay inside these ranges and needn't reach their ends.
There are 2 independent parts, one for each index of `groups`. The reference program is written for one: setup_inputs(seed, part) draws one part's arguments, and reference() takes and returns one part's arrays. A program takes and returns all parts, laid end to end along the dimension named above; an argument that names none is the same for every part. Nothing has to cross between parts.
Inputs may be any that keep to these rules, and one draw needn't show every extreme that they name: `cache_lengths`: each sequence's cached tokens fill the first cache positions; some sequence has exactly 2048.
All inputs are finite; a program needn't handle non-finite values.
Results may differ from the reference program's by a relative error of at most 0.04.
Values may be sent and summed in bfloat16 or wider, within the bound.
A program may use at most 64 MiB of HBM per device.

```python
import math
import jax
import jax.numpy as jnp
from jax import lax

D = 8192
HEADS = 64
KVH = 8
HD = 128
FF = 14336
DRAFT = 16
CTX = 2048
SEQS = 32
ROWS = 512
N_FFN = 32
N_HIDDEN = 8


def draw_residual_in(key, part):
    ramp = 0.6 + 1.4 * jnp.arange(D).astype(jnp.float32) / D
    base = jnp.clip(jax.random.normal(key, (ROWS, D), jnp.float32), -5.0, 5.0)
    return (base * ramp[None, :]).astype(jnp.bfloat16)


def draw_queries(key, part):
    base = jnp.clip(jax.random.normal(key, (ROWS, HEADS * HD), jnp.float32), -4.0, 4.0)
    return base.astype(jnp.bfloat16)


def draw_cache_lengths(key, part):
    first_key, second_key = jax.random.split(jax.random.fold_in(key, 3))
    drawn = jax.random.randint(first_key, (SEQS,), 1, CTX + 1)
    chosen_seq = jax.random.randint(second_key, (), 0, SEQS)
    return jnp.where(jnp.arange(SEQS) == chosen_seq, CTX, drawn).astype(jnp.int32)


def level_of(key, extent, cuts, least, top_value):
    def one(dim, blocks):
        draws = jax.random.uniform(jax.random.fold_in(jax.random.fold_in(key, 6), dim), (blocks,), jnp.float32, least / len(cuts), top_value / len(cuts))
        return jnp.repeat(jnp.exp(draws), extent[dim] // blocks).reshape((-1,) + (1,) * (len(extent) - dim - 1))

    gain = one(*cuts[0])
    for cut in cuts[1:]:
        gain = gain * one(*cut)
    return gain


def gaussian(own_key, extent, deviation, limit, shards=(), kind=jnp.bfloat16):
    entries = jax.random.normal(own_key, extent, jnp.float32) * deviation
    if len(shards) > 0:
        entries = level_of(own_key, extent, shards, -0.22, 0.18) * entries
    return jnp.clip(entries, min=-limit, max=limit).astype(kind)


def setup_inputs(seed: int = 0, part: int = 0) -> dict:
    key_of = jax.random.split(jax.random.key(seed), 13)
    part_splits = jax.random.split(jax.random.fold_in(key_of[12], part), 13)
    return {
        "residual_in": draw_residual_in(jax.random.fold_in(jax.random.fold_in(key_of[12], part), 71), part),
        "queries": draw_queries(jax.random.fold_in(jax.random.fold_in(key_of[12], part), 71), part),
        "new_keys": gaussian(part_splits[2], (ROWS, KVH * HD), 1.0, 6.0, ((0, 8), (1, 32))),
        "new_values": gaussian(part_splits[3], (ROWS, KVH * HD), 4.0, 24.0, ((0, 8), (1, 32))),
        "key_cache": gaussian(part_splits[4], (SEQS, CTX, KVH * HD), 1.0, 6.0, ((0, 8), (1, 32))),
        "value_cache": gaussian(part_splits[5], (SEQS, CTX, KVH * HD), 4.0, 24.0, ((0, 8), (1, 32))),
        "cache_lengths": draw_cache_lengths(jax.random.fold_in(jax.random.fold_in(key_of[12], part), 71), part),
        "norm_gain": jnp.clip(1.0 + 0.18 * jax.random.normal(key_of[7], (D,), jnp.float32), 0.099609375, 1.8984375).astype(jnp.bfloat16),
        "out_weight": gaussian(key_of[8], (HEADS * HD, D), (HEADS * HD // 16) ** -0.5, 0.25, ((0, 32), (1, 8))),
        "gate_weight": gaussian(key_of[9], (D, FF), (D // 4) ** -0.5, 0.125, ((0, 8), (1, 32))),
        "up_weight": gaussian(key_of[10], (D, FF), (D // 4) ** -0.5, 0.125, ((0, 8), (1, 32))),
        "down_weight": gaussian(key_of[11], (FF, D), (FF // 4) ** -0.5, 0.09375, ((0, 32), (1, 8))),
    }


def rope_tables(positions):
    steps_half = jnp.arange(HD // 2).astype(jnp.float32)
    inverse = jnp.exp(steps_half * (-2.0 * math.log(500000.0) / HD))
    angle = positions.astype(jnp.float32)[:, None] * inverse[None, :]
    return (jnp.cos(angle), jnp.sin(angle))

def rotate(values, cosine, sine_table):
    half = values.shape[-1] // 2
    first_half = values[..., :half]
    second_half = values[..., half:]
    cosine = cosine[:, None, :]
    sine_table = sine_table[:, None, :]
    return jnp.concatenate([first_half * cosine - second_half * sine_table, second_half * cosine + first_half * sine_table], axis=-1)

def rounded(values):
    return lax.optimization_barrier(values.astype(jnp.bfloat16)).astype(jnp.float32)

def one_sequence(inputs):
    queries, new_keys, new_values, key_cache, value_cache, length = inputs
    group = HEADS // KVH
    block = CTX // N_FFN
    positions = length + jnp.arange(DRAFT, dtype=jnp.int32)
    cosine, sine_table = rope_tables(positions)
    query_rot = rounded(rotate(queries.astype(jnp.float32).reshape(DRAFT, HEADS, HD), cosine, sine_table))
    query_rot = query_rot.reshape(DRAFT, KVH, group, HD)
    key_rot = rounded(rotate(new_keys.astype(jnp.float32).reshape(DRAFT, KVH, HD), cosine, sine_table))
    cached_keys = key_cache.astype(jnp.float32).reshape(CTX, KVH, HD)
    scaling = 1.0 / math.sqrt(HD)
    cache_scores = jnp.einsum('jkgd,pkd->jkgp', query_rot, cached_keys) * scaling
    draft_scores = jnp.einsum('jkgd,ikd->jkgi', query_rot, key_rot) * scaling
    usable = jnp.arange(CTX) < length
    causal = (jnp.arange(DRAFT)[None, :] <= jnp.arange(DRAFT)[:, None])[:, None, None, :]
    cache_scores = jnp.where(usable, cache_scores, -1e+30)
    draft_scores = jnp.where(causal, draft_scores, -1e+30)
    peak_score = jnp.maximum(cache_scores.max(-1), draft_scores.max(-1))[..., None]
    cache_weights = jnp.where(usable, jnp.exp(cache_scores - peak_score), 0.0)
    draft_weights = jnp.where(causal, jnp.exp(draft_scores - peak_score), 0.0)
    cached_values = value_cache.astype(jnp.float32).reshape(N_FFN, block, KVH, HD)
    block_weights = cache_weights.reshape(DRAFT, KVH, group, N_FFN, block)
    numerator = jnp.einsum('jkgbp,bpkd->bjkgd', rounded(block_weights), cached_values)
    denominator = jnp.moveaxis(block_weights.sum(-1), -1, 0)
    draft_values = new_values.astype(jnp.float32).reshape(DRAFT, KVH, HD)
    numerator = numerator.at[0].add(jnp.einsum('jkgi,ikd->jkgd', rounded(draft_weights), draft_values))
    denominator = denominator.at[0].add(draft_weights.sum(-1))
    numerator = lax.optimization_barrier(jnp.sum(rounded(numerator), axis=0))
    denominator = lax.optimization_barrier(jnp.sum(rounded(denominator), axis=0))
    return (numerator / denominator[..., None]).reshape(DRAFT, HEADS * HD).astype(jnp.bfloat16)

def blockwise(left, right, pieces):
    width = left.shape[1] // pieces

    def add_piece(counter, total):
        offset = (counter * width).astype(jnp.int32)
        left_part = lax.dynamic_slice_in_dim(left, offset, width, 1)
        right_part = lax.dynamic_slice_in_dim(right, offset, width, 0)
        return total + rounded(jnp.dot(left_part, right_part, preferred_element_type=jnp.float32))
    initial = jnp.zeros((left.shape[0], right.shape[1]), jnp.float32)
    return lax.fori_loop(0, pieces, add_piece, initial)

def reference(residual_in, queries, new_keys, new_values, key_cache, value_cache, cache_lengths, norm_gain, out_weight, gate_weight, up_weight, down_weight):
    attended = lax.map(one_sequence, (queries.reshape(SEQS, DRAFT, HEADS * HD), new_keys.reshape(SEQS, DRAFT, KVH * HD), new_values.reshape(SEQS, DRAFT, KVH * HD), key_cache, value_cache, cache_lengths))
    attended = attended.reshape(ROWS, HEADS * HD)
    projected = blockwise(attended, out_weight, N_FFN)
    resid = (residual_in.astype(jnp.float32) + projected).astype(jnp.bfloat16)
    widened = resid.astype(jnp.float32)
    factor = lax.rsqrt(lax.optimization_barrier(jnp.mean(widened * widened, axis=1, keepdims=True)) + 1e-05)
    normed = (widened * factor * norm_gain.astype(jnp.float32)[None, :]).astype(jnp.bfloat16)
    gate = blockwise(normed, gate_weight, N_HIDDEN)
    upward = blockwise(normed, up_weight, N_HIDDEN)
    activation = (jax.nn.silu(gate) * upward).astype(jnp.bfloat16)
    lowered = blockwise(activation, down_weight, N_FFN)
    return (widened + lowered).astype(jnp.bfloat16)
```

```python
import functools
import math

import jax
import jax.numpy as jnp
from jax import lax
from jax.experimental import pallas as pl
from jax.experimental.pallas import tpu as pltpu
from jax.sharding import PartitionSpec as P

HD = 128
DRAFT = 16
FAR = -1e30
FLOOR = -1e29
MESH = pl.DeviceIdType.MESH
F32 = jnp.float32
BF16 = jnp.bfloat16


def iota(shape, dim):
    return lax.broadcasted_iota(jnp.int32, shape, dim)


def tail_of(peak, total):
    high = total.astype(BF16).astype(F32)
    low = total - high
    row = iota((16, peak.shape[1]), 0)
    tile = jnp.where(row == 0, peak, jnp.where(row == 1, high, jnp.where(row == 2, low, 0.0)))
    return tile.astype(BF16)


def merged_state(states):
    peak = functools.reduce(jnp.maximum, [s[1] for s in states])
    numerator, denominator = 0.0, 0.0
    for num, own_peak, den in states:
        factor = jnp.exp(own_peak - peak)
        numerator = numerator + num * factor
        denominator = denominator + den * factor
    return numerator, peak, denominator


def read_state(ref):
    num = ref[pl.ds(0, HD), :].astype(F32)
    tail = ref[pl.ds(HD, 16), :].astype(F32)
    return num, tail[0:1], tail[1:2] + tail[2:3]


def write_state(ref, num, peak, den):
    ref[pl.ds(0, HD), :] = num.astype(BF16)
    ref[pl.ds(HD, 16), :] = tail_of(peak, den)


def kernel(
    nz,
    nh,
    lengths,
    q_own,
    kv_own,
    cosine,
    sine,
    gain,
    residual,
    key_hbm,
    value_hbm,
    wo_hbm,
    wg_hbm,
    wu_hbm,
    wd_hbm,
    out,
    keys,
    values,
    wo,
    wg,
    wu,
    wd,
    load_sem,
    q_all,
    kv_all,
    kv_send,
    kv_recv,
    bias,
    values_t,
    state,
    s_leaf,
    s_chain,
    s_out,
    attended,
    blocks,
    b_leaf,
    b_chain,
    b_out,
    lower,
    l_leaf,
    l_chain,
    l_out,
    resid,
    scaled,
    squares,
    w_in,
    w_down,
    h_send,
    h_recv,
    acts,
    g_send,
    g_recv,
    r_send,
    r_recv,
    x_send,
    x_recv,
):
    z = lax.axis_index("ffn")
    h = lax.axis_index("hidden")
    turn = nz // 4
    rows, seqs, block = attended.shape[1] // 2, keys.shape[0], keys.shape[1]
    kv_heads = keys.shape[2] // HD
    share = nz // kv_heads
    lanes = q_own.shape[0]
    per = nz // nh
    rz, width = residual.shape
    inner = wg.shape[1]
    half = w_in.shape[1] // 2

    def at_z(i):
        return lax.rem(i + nz, nz)

    def at_h(i):
        return lax.rem(i, nh)

    loads = [
        pltpu.make_async_copy(src, dst, load_sem.at[i])
        for i, (src, dst) in enumerate(
            (
                (key_hbm, keys),
                (value_hbm, values),
                (wo_hbm, wo),
                (wg_hbm, wg),
                (wu_hbm, wu),
                (wd_hbm, wd),
            )
        )
    ]
    for load in loads:
        load.start()

    barrier = pltpu.get_barrier_semaphore()
    around = [d for d in range(-(share - 1), share) if d != 0]
    for d in around:
        pl.semaphore_signal(barrier, inc=1, device_id={"ffn": at_z(z + d)}, device_id_type=MESH)
    for d in range(1, nh):
        pl.semaphore_signal(barrier, inc=1, device_id={"hidden": at_h(h + d)}, device_id_type=MESH)
    pl.semaphore_wait(barrier, len(around) + nh - 1)

    def sign(d):
        return 1 if d == 0 else -1

    def gather_tools(buf, own, send, recv):
        def copy(d, far, k, src=None):
            slot = at_z(z - sign(d) * 2 * k)
            return pltpu.make_async_remote_copy(
                src_ref=buf.at[slot] if src is None else src,
                dst_ref=buf.at[slot],
                send_sem=send.at[d, far, k],
                recv_sem=recv.at[d, far, k],
                device_id={"ffn": at_z(z + sign(d) * (1 + far))},
                device_id_type=MESH,
            )

        def arrived(d, far, k):
            slot = at_z(z - sign(d) * (2 * k + 1 + far))
            pltpu.make_async_remote_copy(
                src_ref=buf.at[slot],
                dst_ref=buf.at[slot],
                send_sem=send.at[d, far, k],
                recv_sem=recv.at[d, far, k],
                device_id={"ffn": at_z(z - sign(d) * (1 + far))},
                device_id_type=MESH,
            ).wait_recv()
            return slot

        def first():
            for far in (1, 0):
                for d in (0, 1):
                    copy(d, far, 0, own).start()

        def rest(process):
            def step(k, last):
                there = []
                for d in (0, 1):
                    there.append(arrived(d, 1, k - 1))
                    if not (last and d == 1):
                        copy(d, 1, k).start()
                    copy(d, 0, k).start()
                for slot in there:
                    process(slot)
                for d in (0, 1):
                    process(arrived(d, 0, k - 1))

            @pl.loop(1, turn - 1)
            def _(k):
                step(k, False)

            step(turn - 1, True)
            for d in (0, 1):
                process(arrived(d, 0, turn - 1))
            process(arrived(0, 1, turn - 1))

        def drain():
            for far in (1, 0):
                for d in (0, 1):
                    copy(d, far, 0, own).wait_send()

            @pl.loop(1, turn)
            def _(k):
                copy(0, 1, k).wait_send()
                copy(0, 0, k).wait_send()
                copy(1, 0, k).wait_send()

            @pl.loop(1, turn - 1)
            def _(k):
                copy(1, 1, k).wait_send()

        return first, rest, drain

    def scatter_tools(blk, leaf, chain, stage, which):
        def leaf_copy(d, i):
            return pltpu.make_async_remote_copy(
                src_ref=blk.at[at_z(z + sign(d) * (2 * i + 1))],
                dst_ref=leaf.at[d, i],
                send_sem=r_send.at[which, 0, d, i],
                recv_sem=r_recv.at[which, 0, d, i],
                device_id={"ffn": at_z(z + sign(d))},
                device_id_type=MESH,
            )

        def chain_copy(d, i, src=None):
            return pltpu.make_async_remote_copy(
                src_ref=stage.at[d, i] if src is None else src,
                dst_ref=chain.at[d, i],
                send_sem=r_send.at[which, 1, d, i],
                recv_sem=r_recv.at[which, 1, d, i],
                device_id={"ffn": at_z(z + 2 * sign(d))},
                device_id_type=MESH,
            )

        def start_copy():
            return chain_copy(0, turn - 1, blk.at[at_z(z + 2 * turn)])

        def run(merge):
            start_copy().start()
            for i in (turn - 1, turn - 2):
                for d in (0, 1):
                    leaf_copy(d, i).start()
            top = turn - 1
            leaf_copy(1, top).wait_recv()
            merge([blk.at[at_z(z - 2 * top)], leaf.at[1, top]], stage.at[1, top - 1])
            chain_copy(1, top - 1).start()
            leaf_copy(0, top).wait_recv()
            chain_copy(0, top).wait_recv()
            merge(
                [blk.at[at_z(z + 2 * top)], leaf.at[0, top], chain.at[0, top]],
                stage.at[0, top - 1],
            )
            chain_copy(0, top - 1).start()

            @pl.loop(0, turn - 2)
            def _(t):
                k = turn - 2 - t
                for d in (0, 1):
                    leaf_copy(d, k - 1).start()
                for d in (0, 1):
                    leaf_copy(d, k).wait_recv()
                    chain_copy(d, k).wait_recv()
                    merge(
                        [blk.at[at_z(z + sign(d) * 2 * k)], leaf.at[d, k], chain.at[d, k]],
                        stage.at[d, k - 1],
                    )
                    chain_copy(d, k - 1).start()

            for d in (0, 1):
                leaf_copy(d, 0).wait_recv()
                chain_copy(d, 0).wait_recv()
            return [blk.at[z], leaf.at[0, 0], leaf.at[1, 0], chain.at[0, 0], chain.at[1, 0]]

        def drain():
            start_copy().wait_send()

            @pl.loop(0, turn)
            def _(i):
                leaf_copy(0, i).wait_send()
                leaf_copy(1, i).wait_send()

            @pl.loop(0, turn - 1)
            def _(i):
                chain_copy(0, i).wait_send()
                chain_copy(1, i).wait_send()

        return run, drain

    def peer_copy(which, d, src, dst):
        return pltpu.make_async_remote_copy(
            src_ref=src,
            dst_ref=dst,
            send_sem=x_send.at[which, d],
            recv_sem=x_recv.at[which, d],
            device_id={"hidden": at_h(h + d)},
            device_id_type=MESH,
        )

    q_first, q_rest, q_drain = gather_tools(q_all, q_own, g_send.at[0], g_recv.at[0])
    q_first()

    def kv_copy(d):
        return pltpu.make_async_remote_copy(
            src_ref=kv_own,
            dst_ref=kv_all.at[share - 1 - d],
            send_sem=kv_send.at[d + share - 1],
            recv_sem=kv_recv.at[share - 1 - d],
            device_id={"ffn": at_z(z + d)},
            device_id_type=MESH,
        )

    for d in around:
        kv_copy(d).start()
    q_all[z] = q_own[...]
    kv_all[share - 1] = kv_own[...]

    shape = (seqs * block, lanes)
    row, lane = iota(shape, 0), iota(shape, 1)
    cached_seq, lane_seq = row // block, (lane % rows) // DRAFT
    length = functools.reduce(
        jnp.add, [jnp.where(cached_seq == i, lengths[i], 0) for i in range(seqs)]
    )
    usable = jnp.logical_and(cached_seq == lane_seq, z * block + row % block < length)
    bias[...] = jnp.where(usable, 0.0, FAR)
    scaling = 1.0 / math.sqrt(HD)

    loads[1].wait()

    @pl.loop(0, kv_heads)
    def _(k):
        head = values[:, :, pl.ds(pl.multiple_of(k * HD, HD), HD)].reshape(seqs * block, HD)
        values_t[k] = head.astype(F32).T.astype(BF16)

    loads[0].wait()

    def partial_softmax(scores):
        peak = jnp.maximum(jnp.max(scores, axis=0, keepdims=True), FLOOR)
        peak = peak.astype(BF16).astype(F32)
        weights = jnp.exp(scores - peak)
        return weights, peak, jnp.sum(weights, axis=0, keepdims=True)

    def attend(slot):
        k = slot // share
        head = keys[:, :, pl.ds(pl.multiple_of(k * HD, HD), HD)].reshape(seqs * block, HD)
        scores = lax.dot_general(
            head, q_all[slot], (((1,), (1,)), ((), ())), preferred_element_type=F32
        )
        weights, peak, den = partial_softmax(scores * scaling + bias[...])
        num = jnp.dot(values_t[k], weights.astype(BF16), preferred_element_type=F32)
        write_state(state.at[slot], num, peak, den)

    attend(z)
    q_rest(attend)

    s_run, s_drain = scatter_tools(state, s_leaf, s_chain, s_out, 0)

    def merge_states(refs, dst):
        write_state(dst, *merged_state([read_state(r) for r in refs]))

    last = s_run(merge_states)
    for d in around:
        kv_copy(d).wait_recv()
    quarter = HD // share
    first_of_head = z - z % share
    fresh_k, fresh_v = jnp.zeros((rows, HD), F32), jnp.zeros((rows, HD), F32)
    part = iota((rows, HD), 1) // quarter
    for i in range(share):
        pair = kv_all[first_of_head + i - z + share - 1].astype(F32)
        rolled_k = pair if i == 0 else pltpu.roll(pair, i * quarter, 1)
        shift_v = (i - 1) * quarter % HD
        rolled_v = pair if shift_v == 0 else pltpu.roll(pair, shift_v, 1)
        fresh_k = jnp.where(part == i, rolled_k, fresh_k)
        fresh_v = jnp.where(part == i, rolled_v, fresh_v)
    fresh_k = fresh_k * cosine[...] + pltpu.roll(fresh_k, HD // 2, 1) * sine[...]
    draft_scores = lax.dot_general(
        fresh_k.astype(BF16), q_own[...], (((1,), (1,)), ((), ())), preferred_element_type=F32
    )
    row, lane = iota((rows, lanes), 0), iota((rows, lanes), 1)
    causal = jnp.logical_and(
        row // DRAFT == (lane % rows) // DRAFT, row % DRAFT <= lane % DRAFT
    )
    weights, peak, den = partial_softmax(jnp.where(causal, draft_scores * scaling, FAR))
    num = jnp.dot(fresh_v.T.astype(BF16), weights.astype(BF16), preferred_element_type=F32)
    num, peak, den = merged_state([read_state(r) for r in last] + [(num, peak, den)])
    attended[h] = (num / den).T.astype(BF16)

    for d in range(1, nh):
        peer_copy(0, d, attended.at[h], attended.at[h]).start()
    loads[2].wait()

    def project(c):
        pair = attended[c]
        both = jnp.concatenate([pair[:rows], pair[rows:]], axis=1)
        product = jnp.dot(both, wo[...], preferred_element_type=F32).astype(BF16)
        blocks[pl.ds(c * per, per)] = product.reshape(per, rz, width)

    project(h)

    @pl.loop(1, nh)
    def _(d):
        src = at_h(h + nh - d)
        peer_copy(0, d, attended.at[src], attended.at[src]).wait_recv()
        project(src)

    p_run, p_drain = scatter_tools(blocks, b_leaf, b_chain, b_out, 1)

    def total(refs):
        return functools.reduce(jnp.add, [r[...].astype(F32) for r in refs])

    def add(refs, dst):
        dst[...] = total(refs).astype(BF16)

    last = p_run(add)
    resid[z] = (residual[...].astype(F32) + total(last)).astype(BF16)

    n_first, n_rest, n_drain = gather_tools(resid, resid.at[z], g_send.at[1], g_recv.at[1])
    n_first()
    for load in loads[3:]:
        load.wait()
    w_in[:, pl.ds(half - HD, HD)] = jnp.zeros((width, HD), BF16)
    w_in[:, pl.ds(2 * half - HD, HD)] = jnp.zeros((width, HD), BF16)
    w_in[:, pl.ds(0, inner)] = wg[...]
    w_in[:, pl.ds(half, inner)] = wu[...]
    w_down[pl.ds(0, inner), :] = wd[...]
    w_down[pl.ds(inner, half - inner), :] = jnp.zeros((half - inner, width), BF16)
    gains = gain[...].astype(F32)

    def scale(slot):
        values_here = resid[slot].astype(F32)
        ssq = jnp.sum(values_here * values_here, axis=1, keepdims=True)
        squares[slot] = jnp.broadcast_to(ssq, (rz, HD))
        scaled[slot] = (values_here * gains).astype(BF16)

    scale(z)
    n_rest(scale)

    def inner_sums(c):
        lhs = scaled[pl.ds(c * per, per)].reshape(rows, width)
        sums = jnp.dot(lhs, w_in[...], preferred_element_type=F32)
        ssq = squares[pl.ds(c * per, per)].reshape(rows, HD)
        high = ssq.astype(BF16).astype(F32)
        column = iota((rows, HD), 1)
        extra = jnp.where(
            column == HD - 2, high, jnp.where(column == HD - 1, ssq - high, 0.0)
        )
        h_send[c, :, pl.ds(0, half - HD)] = sums[:, : half - HD].astype(BF16)
        h_send[c, :, pl.ds(half - HD, HD)] = (sums[:, half - HD : half] + extra).astype(BF16)
        h_send[c, :, pl.ds(half, half)] = sums[:, half:].astype(BF16)

    @pl.loop(1, nh)
    def _(d):
        c = at_h(h + d)
        inner_sums(c)
        peer_copy(1, d, h_send.at[c], h_recv.at[h]).start()

    inner_sums(h)
    h_recv[h] = h_send[h]

    @pl.loop(1, nh)
    def _(d):
        src = at_h(h + nh - d)
        peer_copy(1, d, h_recv.at[src], h_recv.at[src]).wait_recv()

    sums = total([h_recv.at[i] for i in range(nh)])
    edge = sums[:, half - HD : half]
    ssq = jnp.sum(jnp.where(iota((rows, HD), 1) >= HD - 2, edge, 0.0), axis=1, keepdims=True)
    factor = lax.rsqrt(ssq / (nh * width) + 1e-05)
    gate, up = sums[:, :half] * factor, sums[:, half:] * factor
    gate = jnp.where(iota((rows, half), 1) < inner, gate, 0.0)
    acts[h] = (gate / (1.0 + jnp.exp(-gate)) * up).astype(BF16)

    for d in range(1, nh):
        peer_copy(2, d, acts.at[h], acts.at[h]).start()

    def descend(c):
        product = jnp.dot(acts[c], w_down[...], preferred_element_type=F32).astype(BF16)
        lower[pl.ds(c * per, per)] = product.reshape(per, rz, width)

    descend(h)

    @pl.loop(1, nh)
    def _(d):
        src = at_h(h + nh - d)
        peer_copy(2, d, acts.at[src], acts.at[src]).wait_recv()
        descend(src)

    d_run, d_drain = scatter_tools(lower, l_leaf, l_chain, l_out, 2)
    last = d_run(add)
    out[...] = (resid[z].astype(F32) + total(last)).astype(BF16)

    q_drain()
    for d in around:
        kv_copy(d).wait_send()
    s_drain()
    p_drain()
    n_drain()
    d_drain()

    @pl.loop(1, nh)
    def _(d):
        c = at_h(h + d)
        peer_copy(0, d, attended.at[h], attended.at[h]).wait_send()
        peer_copy(1, d, h_send.at[c], h_recv.at[h]).wait_send()
        peer_copy(2, d, acts.at[h], acts.at[h]).wait_send()


def shards(
    residual_in,
    queries,
    new_keys,
    new_values,
    key_cache,
    value_cache,
    cache_lengths,
    norm_gain,
    out_weight,
    gate_weight,
    up_weight,
    down_weight,
):
    nz, nh = lax.axis_size("ffn"), lax.axis_size("hidden")
    rows, columns = queries.shape
    heads = columns // HD
    seqs, block, kv_width = key_cache.shape
    kv_heads = kv_width // HD
    share = nz // kv_heads
    rz, width = residual_in.shape
    inner = gate_weight.shape[1]
    half = -(-(inner + 2) // HD) * HD
    turn = nz // 4
    lanes = heads * rows
    positions = (cache_lengths[:, None] + jnp.arange(DRAFT, dtype=jnp.int32)[None, :]).reshape(-1)
    steps_half = jnp.arange(HD // 2).astype(F32)
    inverse = jnp.exp(steps_half * (-2.0 * math.log(500000.0) / HD))
    angle = positions.astype(F32)[:, None] * inverse[None, :]
    cosine, sine = jnp.cos(angle), jnp.sin(angle)
    both_cosine = jnp.concatenate([cosine, cosine], axis=1)
    both_sine = jnp.concatenate([-sine, sine], axis=1)
    q = queries.astype(F32).reshape(rows, heads, HD).transpose(1, 0, 2)
    swapped = jnp.concatenate([q[..., HD // 2 :], q[..., : HD // 2]], axis=-1)
    q_rot = (q * both_cosine + swapped * both_sine).astype(BF16).reshape(lanes, HD)
    quarter = new_keys.shape[1]
    pad = jnp.zeros((rows, HD - 2 * quarter), BF16)
    kv = jnp.concatenate([new_keys, new_values, pad], axis=1)
    vmem = pl.BlockSpec(memory_space=pltpu.VMEM)
    anywhere = pl.BlockSpec(memory_space=pl.ANY)
    dma = pltpu.SemaphoreType.DMA
    extent = HD + 16

    def scatter_buffers(shape):
        return [pltpu.VMEM((2, turn, *shape), BF16)] * 3

    scratch = [
        pltpu.VMEM(key_cache.shape, BF16),
        pltpu.VMEM(value_cache.shape, BF16),
        pltpu.VMEM(out_weight.shape, BF16),
        pltpu.VMEM(gate_weight.shape, BF16),
        pltpu.VMEM(up_weight.shape, BF16),
        pltpu.VMEM(down_weight.shape, BF16),
        dma((6,)),
        pltpu.VMEM((nz, lanes, HD), BF16),
        pltpu.VMEM((2 * share - 1, rows, HD), BF16),
        dma((2 * share - 1,)),
        dma((2 * share - 1,)),
        pltpu.VMEM((seqs * block, lanes), F32),
        pltpu.VMEM((kv_heads, HD, seqs * block), BF16),
        pltpu.VMEM((nz, extent, lanes), BF16),
        *scatter_buffers((extent, lanes)),
        pltpu.VMEM((nh, lanes, HD), BF16),
        pltpu.VMEM((nz, rz, width), BF16),
        *scatter_buffers((rz, width)),
        pltpu.VMEM((nz, rz, width), BF16),
        *scatter_buffers((rz, width)),
        pltpu.VMEM((nz, rz, width), BF16),
        pltpu.VMEM((nz, rz, width), BF16),
        pltpu.VMEM((nz, rz, HD), F32),
        pltpu.VMEM((width, 2 * half), BF16),
        pltpu.VMEM((half, width), BF16),
        pltpu.VMEM((nh, rows, 2 * half), BF16),
        pltpu.VMEM((nh, rows, 2 * half), BF16),
        pltpu.VMEM((nh, rows, half), BF16),
        dma((2, 2, 2, turn)),
        dma((2, 2, 2, turn)),
        dma((3, 2, 2, turn)),
        dma((3, 2, 2, turn)),
        dma((3, nh)),
        dma((3, nh)),
    ]
    return pl.pallas_call(
        functools.partial(kernel, nz, nh),
        out_shape=jax.ShapeDtypeStruct(residual_in.shape, BF16),
        in_specs=[pl.BlockSpec(memory_space=pltpu.SMEM)] + [vmem] * 6 + [anywhere] * 6,
        out_specs=vmem,
        scratch_shapes=scratch,
        compiler_params=pltpu.CompilerParams(
            collective_id=0, has_side_effects=True, vmem_limit_bytes=60 * 1024 * 1024
        ),
        name="block_step",
    )(
        cache_lengths,
        q_rot,
        kv,
        both_cosine,
        both_sine,
        norm_gain[None, :],
        residual_in,
        key_cache,
        value_cache,
        out_weight,
        gate_weight,
        up_weight,
        down_weight,
    )


def solution(mesh):
    in_specs = (
        P(("groups", "ffn"), "hidden"),
        P(("groups", "hidden"), "ffn"),
        P(("groups", "hidden"), "ffn"),
        P(("groups", "hidden"), "ffn"),
        P(("groups", "hidden"), "ffn", None),
        P(("groups", "hidden"), "ffn", None),
        P(("groups", "hidden")),
        P("hidden"),
        P("ffn", "hidden"),
        P("hidden", "ffn"),
        P("hidden", "ffn"),
        P("ffn", "hidden"),
    )
    out_specs = P(("groups", "ffn"), "hidden")
    return jax.shard_map(shards, mesh=mesh, in_specs=in_specs, out_specs=out_specs, check_vma=False)
```

```python
import functools
import math

import jax
import jax.numpy as jnp
from jax import lax
from jax.experimental import pallas as pl
from jax.experimental.pallas import tpu as pltpu
from jax.sharding import PartitionSpec as P

HD = 128
DRAFT = 16
GATHER = 3
SCATTER = 3
BATCH = 8
FAR = -1e30
FLOOR = -1e29
MESH = pl.DeviceIdType.MESH
F32 = jnp.float32
BF16 = jnp.bfloat16


def iota(shape, dim):
    return lax.broadcasted_iota(jnp.int32, shape, dim)


class Tree:
    def __init__(self, n, stride):
        self.stride = stride
        self.parent = {}
        for side, most in ((1, n // 2), (-1, n // 2 - 1)):
            for d in range(1, most + 1):
                over = d % stride
                up = d - over + stride
                if over == 0:
                    self.parent[side * d] = side * (d - stride)
                elif stride - over < over and up <= most:
                    self.parent[side * d] = side * up
                else:
                    self.parent[side * d] = side * (d - over)
        self.kids = {x: [] for x in [0, *self.parent]}
        for x, p in self.parent.items():
            self.kids[p].append(x)
        for x in self.kids:
            self.kids[x].sort(key=lambda y: (-len(self.kids[y]), -abs(self.hop(y)), y))
        self.order = sorted(self.parent, key=lambda x: (self.level(x), abs(x), x))
        self.index = {x: i for i, x in enumerate(sorted(self.parent))}

    def hop(self, x):
        return x - self.parent[x]

    def level(self, x):
        if abs(x) % self.stride == 0:
            return 2 * abs(x) // self.stride
        return self.level(self.parent[x]) + 3


def tail_of(peak, total):
    high = total.astype(BF16).astype(F32)
    low = total - high
    row = iota((16, peak.shape[1]), 0)
    tile = jnp.where(row == 0, peak, jnp.where(row == 1, high, jnp.where(row == 2, low, 0.0)))
    return tile.astype(BF16)


def merged_state(states):
    peak = functools.reduce(jnp.maximum, [s[1] for s in states])
    numerator, denominator = 0.0, 0.0
    for num, own_peak, den in states:
        factor = jnp.exp(own_peak - peak)
        numerator = numerator + num * factor
        denominator = denominator + den * factor
    return numerator, peak, denominator


def read_state(ref):
    num = ref[pl.ds(0, HD), :].astype(F32)
    tail = ref[pl.ds(HD, 16), :].astype(F32)
    return num, tail[0:1], tail[1:2] + tail[2:3]


def write_state(ref, num, peak, den):
    ref[pl.ds(0, HD), :] = num.astype(BF16)
    ref[pl.ds(HD, 16), :] = tail_of(peak, den)


def partial_softmax(scores):
    peak = jnp.maximum(jnp.max(scores, axis=0, keepdims=True), FLOOR)
    peak = peak.astype(BF16).astype(F32)
    weights = jnp.exp(scores - peak)
    return weights, peak, jnp.sum(weights, axis=0, keepdims=True)


def kernel(
    nz,
    nh,
    gather,
    scatter,
    lengths,
    queries,
    fresh_k,
    fresh_v,
    gain,
    residual,
    key_hbm,
    value_hbm,
    wo_hbm,
    wg_hbm,
    wu_hbm,
    wd_hbm,
    out,
    keys,
    values,
    wo,
    w_in,
    w_down,
    load_sem,
    q_all,
    kv_all,
    kv_send,
    kv_recv,
    bias,
    values_t,
    state,
    s_in,
    s_out,
    attended,
    blocks,
    b_in,
    b_out,
    lower,
    l_in,
    l_out,
    resid,
    scaled,
    squares,
    h_send,
    h_recv,
    acts,
    z_send,
    z_recv,
    x_send,
    x_recv,
    e_send,
    e_recv,
):
    z = lax.axis_index("ffn")
    h = lax.axis_index("hidden")
    rows, columns = queries.shape
    seqs, block = keys.shape[0], keys.shape[1]
    kv_heads = keys.shape[2] // HD
    share = nz // kv_heads
    lanes = rows * columns // HD
    per = nz // nh
    rz, width = residual.shape
    inner = wg_hbm.shape[0]
    half = w_in.shape[0] // 2
    batches = nz // BATCH
    group = BATCH // nh

    def at_z(i):
        return lax.rem(i + nz, nz)

    def at_h(i):
        return lax.rem(i + nh, nh)

    loads = [
        pltpu.make_async_copy(src, dst, load_sem.at[i])
        for i, (src, dst) in enumerate(
            (
                (key_hbm, keys),
                (value_hbm, values),
                (wo_hbm, wo),
                (wg_hbm, w_in.at[pl.ds(0, inner)]),
                (wu_hbm, w_in.at[pl.ds(half, inner)]),
                (wd_hbm, w_down.at[pl.ds(0, inner)]),
            )
        )
    ]
    for load in loads:
        load.start()

    barrier = pltpu.get_barrier_semaphore()
    reach = max(share - 1, GATHER, SCATTER)
    around = [d for d in range(-reach, reach + 1) if d != 0]
    for d in around:
        pl.semaphore_signal(barrier, inc=1, device_id={"ffn": at_z(z + d)}, device_id_type=MESH)
    for d in range(1, nh):
        pl.semaphore_signal(barrier, inc=1, device_id={"hidden": at_h(h + d)}, device_id_type=MESH)

    row, lane = iota((rows, HD), 0), iota((rows, HD), 1)
    position = functools.reduce(
        jnp.add, [jnp.where(row // DRAFT == i, lengths[i], 0) for i in range(seqs)]
    )
    position = position + row % DRAFT
    steps = (lane % (HD // 2)).astype(F32)
    angle = position.astype(F32) * jnp.exp(steps * (-2.0 * math.log(500000.0) / HD))
    cosine = jnp.cos(angle)
    sine = jnp.sin(angle)
    sine = jnp.where(lane < HD // 2, -sine, sine)

    def rotate(x):
        return (x * cosine + pltpu.roll(x, HD // 2, 1) * sine).astype(BF16)

    for i in range(columns // HD):
        part = queries[:, pl.ds(i * HD, HD)].astype(F32)
        q_all[z, pl.ds(i * rows, rows), :] = rotate(part)

    shape = (seqs * block, lanes)
    row, lane = iota(shape, 0), iota(shape, 1)
    cached_seq, lane_seq = row // block, (lane % rows) // DRAFT
    length = functools.reduce(
        jnp.add, [jnp.where(cached_seq == i, lengths[i], 0) for i in range(seqs)]
    )
    usable = jnp.logical_and(cached_seq == lane_seq, z * block + row % block < length)
    bias[...] = jnp.where(usable, 0.0, FAR)
    for i in (0, 1):
        kv_all[i, share - 1] = (fresh_k, fresh_v)[i][...]
    pl.semaphore_wait(barrier, len(around) + nh - 1)

    def gather_tools(buf, which):
        def copy(x):
            p = gather.parent[x]
            slot = at_z(z - p)
            return pltpu.make_async_remote_copy(
                src_ref=buf.at[slot],
                dst_ref=buf.at[slot],
                send_sem=z_send.at[which, gather.index[x]],
                recv_sem=z_recv.at[which, gather.index[x]],
                device_id={"ffn": at_z(z + x - p)},
                device_id_type=MESH,
            )

        def arrived(x):
            slot = at_z(z - x)
            pltpu.make_async_remote_copy(
                src_ref=buf.at[slot],
                dst_ref=buf.at[slot],
                send_sem=z_send.at[which, gather.index[x]],
                recv_sem=z_recv.at[which, gather.index[x]],
                device_id={"ffn": at_z(z + gather.parent[x] - x)},
                device_id_type=MESH,
            ).wait_recv()

        def first():
            for x in gather.kids[0]:
                copy(x).start()

        def rest(size, process):
            missing = [
                {-d % nz for side in (0, 1) for d in span_of(t, size, side)}
                for t in range(nz // (2 * size))
            ]
            missing[0].discard(0)
            for x in gather.order:
                arrived(x)
                for y in gather.kids[x]:
                    copy(y).start()
                for t, labels in enumerate(missing):
                    if x % nz in labels:
                        labels.discard(x % nz)
                        if not labels:
                            process(t)

        def drain():
            for x in gather.order:
                copy(x).wait_send()

        return first, rest, drain

    def span_of(t, size, side):
        if side == 0:
            return range(size * t, size * (t + 1))
        return range(-size * (t + 1), -size * t)

    def offset_in(t, size, i):
        return jnp.where(i < size, size * t + i, -size * (t + 1) + i - size)

    def scatter_tools(blk, incoming, staged, which):
        inside = [x for x in scatter.order if scatter.kids[x]]
        stage = {x: i for i, x in enumerate(inside)}

        def copy(x):
            own = blk.at[at_z(z - x)] if x not in stage else staged.at[stage[x]]
            return pltpu.make_async_remote_copy(
                src_ref=own,
                dst_ref=incoming.at[scatter.index[x]],
                send_sem=z_send.at[which, scatter.index[x]],
                recv_sem=z_recv.at[which, scatter.index[x]],
                device_id={"ffn": at_z(z + scatter.parent[x] - x)},
                device_id_type=MESH,
            )

        def gathered(x):
            terms = [blk.at[at_z(z - x)]]
            for y in scatter.kids[x]:
                copy(y).wait_recv()
                terms.append(incoming.at[scatter.index[y]])
            return terms

        def run(merge, before=lambda distance: None):
            for x in reversed(scatter.order):
                before(abs(x))
                if x in stage:
                    merge(gathered(x), staged.at[stage[x]])
                copy(x).start()
            before(0)
            return gathered(0)

        def drain():
            for x in scatter.order:
                copy(x).wait_send()

        return run, drain

    def peer_copy(send, recv, d, src, dst):
        return pltpu.make_async_remote_copy(
            src_ref=src,
            dst_ref=dst,
            send_sem=send.at[d],
            recv_sem=recv.at[d],
            device_id={"hidden": at_h(h + d)},
            device_id_type=MESH,
        )

    q_first, q_rest, q_drain = gather_tools(q_all, 0)
    q_first()
    near = [d for d in range(-(share - 1), share) if d != 0]

    def kv_copy(i, d):
        return pltpu.make_async_remote_copy(
            src_ref=(fresh_k, fresh_v)[i],
            dst_ref=kv_all.at[i, share - 1 - d],
            send_sem=kv_send.at[i, d + share - 1],
            recv_sem=kv_recv.at[i, share - 1 - d],
            device_id={"ffn": at_z(z + d)},
            device_id_type=MESH,
        )

    for d in near:
        for i in (0, 1):
            kv_copy(i, d).start()
    scaling = 1.0 / math.sqrt(HD)
    loads[1].wait()

    @pl.loop(0, kv_heads)
    def _(k):
        head = values[:, :, pl.ds(pl.multiple_of(k * HD, HD), HD)].reshape(seqs * block, HD)
        values_t[k] = head.astype(F32).T.astype(BF16)

    loads[0].wait()

    def attend(t):
        @pl.loop(0, 4)
        def _(i):
            slot = at_z(z + offset_in(t, 2, i))
            k = slot // share
            head = keys[:, :, pl.ds(pl.multiple_of(k * HD, HD), HD)].reshape(seqs * block, HD)
            scores = lax.dot_general(
                head, q_all[slot], (((1,), (1,)), ((), ())), preferred_element_type=F32
            )
            weights, peak, den = partial_softmax(scores * scaling + bias[...])
            num = jnp.dot(values_t[k], weights.astype(BF16), preferred_element_type=F32)
            write_state(state.at[slot], num, peak, den)

    q_rest(2, attend)

    for i in (0, 1):
        for d in near:
            kv_copy(i, d).wait_recv()
    first_of_head = share - 1 - z % share
    fresh = [
        jnp.concatenate([kv_all[i, first_of_head + j] for j in range(share)], axis=0)
        for i in (0, 1)
    ]
    draft_scores = lax.dot_general(
        rotate(fresh[0].astype(F32).T),
        q_all[z],
        (((1,), (1,)), ((), ())),
        preferred_element_type=F32,
    )
    row, lane = iota((rows, lanes), 0), iota((rows, lanes), 1)
    causal = jnp.logical_and(
        row // DRAFT == (lane % rows) // DRAFT, row % DRAFT <= lane % DRAFT
    )

    def merge_states(refs, dst):
        write_state(dst, *merged_state([read_state(r) for r in refs]))

    s_run, s_drain = scatter_tools(state, s_in, s_out, 1)
    last = s_run(merge_states)
    weights, peak, den = partial_softmax(jnp.where(causal, draft_scores * scaling, FAR))
    num = jnp.dot(fresh[1], weights.astype(BF16), preferred_element_type=F32)
    num, peak, den = merged_state([read_state(r) for r in last] + [(num, peak, den)])
    attended[h] = (num / den).T.astype(BF16)

    for d in range(1, nh):
        peer_copy(x_send, x_recv, d, attended.at[h], attended.at[h]).start()
    loads[2].wait()

    def project(c):
        d = at_h(h - c)

        @pl.when(d != 0)
        def _():
            peer_copy(x_send, x_recv, d, attended.at[c], attended.at[c]).wait_recv()

        pair = attended[c]
        both = jnp.concatenate([pair[:rows], pair[rows:]], axis=1)
        product = jnp.dot(both, wo[...], preferred_element_type=F32).astype(BF16)
        blocks[pl.ds(c * per, per)] = product.reshape(per, rz, width)

    done = set()
    center = z // per

    def project_for(distance):
        for j in range(nh // 2, distance // per - 1, -1):
            if j not in done:
                done.add(j)
                project(at_h(center + j))
                if 0 < j < nh // 2:
                    project(at_h(center - j))

    project_for(nz // 2 - 1)

    def total(refs):
        return functools.reduce(jnp.add, [r[...].astype(F32) for r in refs])

    def add(refs, dst):
        dst[...] = total(refs).astype(BF16)

    p_run, p_drain = scatter_tools(blocks, b_in, b_out, 2)
    last = p_run(add, project_for)
    resid[z] = (residual[...].astype(F32) + total(last)).astype(BF16)

    n_first, n_rest, n_drain = gather_tools(resid, 3)
    n_first()
    for load in loads[3:]:
        load.wait()
    gap = half - inner
    w_in[pl.ds(inner, gap), :] = jnp.zeros((gap, width), BF16)
    w_in[pl.ds(half + inner, gap), :] = jnp.zeros((gap, width), BF16)
    w_down[pl.ds(inner, gap), :] = jnp.zeros((gap, width), BF16)

    def inner_sums(t):
        @pl.loop(0, BATCH)
        def _(i):
            slot = at_z(z + offset_in(t, BATCH // 2, i))
            x = resid[slot].astype(F32)
            ssq = jnp.sum(x * x, axis=1, keepdims=True)
            squares[t, i] = jnp.broadcast_to(ssq, (rz, HD))
            for j in range(width // HD):
                cut = slice(j * HD, (j + 1) * HD)
                factor = gain[pl.ds(j, 1), :].astype(F32)
                scaled[t, i, :, pl.ds(j * HD, HD)] = (x[:, cut] * factor).astype(BF16)

        lhs = scaled[t].reshape(BATCH * rz, width)
        sums = lax.dot_general(
            lhs, w_in[...], (((1,), (1,)), ((), ())), preferred_element_type=F32
        )
        ssq = squares[t].reshape(BATCH * rz, HD)
        high = ssq.astype(BF16).astype(F32)
        column = iota((BATCH * rz, HD), 1)
        extra = jnp.where(column == HD - 2, high, jnp.where(column == HD - 1, ssq - high, 0.0))
        for at, size, piece in (
            (0, half - HD, sums[:, : half - HD]),
            (half - HD, HD, sums[:, half - HD : half] + extra),
            (half, half, sums[:, half:]),
        ):
            h_send[t, :, :, pl.ds(at, size)] = piece.astype(BF16).reshape(nh, group * rz, size)
        h_recv[t, h] = h_send[t, h]
        for d in range(1, nh):
            gate_copy(t, d).start()

    def gate_copy(t, d):
        return peer_copy(
            e_send.at[0, t], e_recv.at[0, t], d, h_send.at[t, at_h(h + d)], h_recv.at[t, h]
        )

    def activate(t):
        for d in range(1, nh):
            peer = at_h(h - d)
            peer_copy(
                e_send.at[0, t], e_recv.at[0, t], d, h_recv.at[t, peer], h_recv.at[t, peer]
            ).wait_recv()
        sums = total([h_recv.at[t, i] for i in range(nh)])
        edge = sums[:, half - HD : half]
        lane = iota(edge.shape, 1)
        ssq = jnp.sum(jnp.where(lane >= HD - 2, edge, 0.0), axis=1, keepdims=True)
        factor = lax.rsqrt(ssq / (nh * width) + 1e-05)
        gate, up = sums[:, :half] * factor, sums[:, half:] * factor
        gate = jnp.where(iota(gate.shape, 1) < inner, gate, 0.0)
        acts[t, h] = (gate / (1.0 + jnp.exp(-gate)) * up).astype(BF16)
        for d in range(1, nh):
            act_copy(t, d).start()

    def act_copy(t, d):
        return peer_copy(e_send.at[1, t], e_recv.at[1, t], d, acts.at[t, h], acts.at[t, h])

    def descend(t):
        for d in range(1, nh):
            peer = at_h(h - d)
            peer_copy(
                e_send.at[1, t], e_recv.at[1, t], d, acts.at[t, peer], acts.at[t, peer]
            ).wait_recv()
        lhs = acts[t].reshape(BATCH * rz, half)
        product = jnp.dot(lhs, w_down[...], preferred_element_type=F32).astype(BF16)
        product = product.reshape(BATCH, rz, width)
        for i in range(BATCH):
            lower[at_z(z + offset_in(t, BATCH // 2, i))] = product[i]

    def stages(t):
        inner_sums(t)
        if t >= 1:
            activate(t - 1)
        if t >= 2:
            descend(t - 2)

    n_rest(BATCH // 2, stages)
    if batches >= 2:
        descend(batches - 2)
    activate(batches - 1)
    descend(batches - 1)
    d_run, d_drain = scatter_tools(lower, l_in, l_out, 4)
    last = d_run(add)
    out[...] = (resid[z].astype(F32) + total(last)).astype(BF16)

    q_drain()
    for d in near:
        for i in (0, 1):
            kv_copy(i, d).wait_send()
    s_drain()
    p_drain()
    n_drain()
    d_drain()
    for d in range(1, nh):
        peer_copy(x_send, x_recv, d, attended.at[h], attended.at[h]).wait_send()
        for t in range(batches):
            gate_copy(t, d).wait_send()
            act_copy(t, d).wait_send()


def shards(
    residual_in,
    queries,
    new_keys,
    new_values,
    key_cache,
    value_cache,
    cache_lengths,
    norm_gain,
    out_weight,
    gate_weight,
    up_weight,
    down_weight,
):
    nz, nh = lax.axis_size("ffn"), lax.axis_size("hidden")
    rows, columns = queries.shape
    seqs, block, kv_width = key_cache.shape
    kv_heads = kv_width // HD
    share = nz // kv_heads
    rz, width = residual_in.shape
    inner = gate_weight.shape[1]
    half = -(-(inner + 2) // HD) * HD
    lanes = columns // HD * rows
    batches = nz // BATCH
    gather, scatter = Tree(nz, GATHER), Tree(nz, SCATTER)
    inside = sum(1 for x in scatter.order if scatter.kids[x])
    vmem = pl.BlockSpec(memory_space=pltpu.VMEM)
    anywhere = pl.BlockSpec(memory_space=pl.ANY)
    dma = pltpu.SemaphoreType.DMA
    extent = HD + 16

    def scatter_buffers(shape):
        return [
            pltpu.VMEM((nz, *shape), BF16),
            pltpu.VMEM((nz - 1, *shape), BF16),
            pltpu.VMEM((inside, *shape), BF16),
        ]

    state_buffers = scatter_buffers((extent, lanes))
    sum_buffers = scatter_buffers((rz, width))
    scratch = [
        pltpu.VMEM(key_cache.shape, BF16),
        pltpu.VMEM(value_cache.shape, BF16),
        pltpu.VMEM(out_weight.shape, BF16),
        pltpu.VMEM((2 * half, width), BF16),
        pltpu.VMEM((half, width), BF16),
        dma((6,)),
        pltpu.VMEM((nz, lanes, HD), BF16),
        pltpu.VMEM((2, 2 * share - 1, HD // share, rows), BF16),
        dma((2, 2 * share - 1)),
        dma((2, 2 * share - 1)),
        pltpu.VMEM((seqs * block, lanes), F32),
        pltpu.VMEM((kv_heads, HD, seqs * block), BF16),
        *state_buffers,
        pltpu.VMEM((nh, lanes, HD), BF16),
        *sum_buffers,
        *sum_buffers,
        pltpu.VMEM((nz, rz, width), BF16),
        pltpu.VMEM((batches, BATCH, rz, width), BF16),
        pltpu.VMEM((batches, BATCH, rz, HD), F32),
        pltpu.VMEM((batches, nh, BATCH // nh * rz, 2 * half), BF16),
        pltpu.VMEM((batches, nh, BATCH // nh * rz, 2 * half), BF16),
        pltpu.VMEM((batches, nh, BATCH // nh * rz, half), BF16),
        dma((5, nz - 1)),
        dma((5, nz - 1)),
        dma((nh,)),
        dma((nh,)),
        dma((2, batches, nh)),
        dma((2, batches, nh)),
    ]
    return pl.pallas_call(
        functools.partial(kernel, nz, nh, gather, scatter),
        out_shape=jax.ShapeDtypeStruct(residual_in.shape, BF16),
        in_specs=[pl.BlockSpec(memory_space=pltpu.SMEM)] + [vmem] * 5 + [anywhere] * 6,
        out_specs=vmem,
        scratch_shapes=scratch,
        compiler_params=pltpu.CompilerParams(
            collective_id=0, has_side_effects=True, vmem_limit_bytes=60 * 1024 * 1024
        ),
        name="block_step",
    )(
        cache_lengths,
        queries,
        new_keys.T,
        new_values.T,
        norm_gain.reshape(-1, HD),
        residual_in,
        key_cache,
        value_cache,
        out_weight,
        gate_weight.T,
        up_weight.T,
        down_weight,
    )


def solution(mesh):
    in_specs = (
        P(("groups", "ffn"), "hidden"),
        P(("groups", "hidden"), "ffn"),
        P(("groups", "hidden"), "ffn"),
        P(("groups", "hidden"), "ffn"),
        P(("groups", "hidden"), "ffn", None),
        P(("groups", "hidden"), "ffn", None),
        P(("groups", "hidden")),
        P("hidden"),
        P("ffn", "hidden"),
        P("hidden", "ffn"),
        P("hidden", "ffn"),
        P("ffn", "hidden"),
    )
    out_specs = P(("groups", "ffn"), "hidden")
    return jax.shard_map(shards, mesh=mesh, in_specs=in_specs, out_specs=out_specs, check_vma=False)
```

```python
import functools
import math

import jax
import jax.numpy as jnp
from jax import lax
from jax.experimental import pallas as pl
from jax.experimental.pallas import tpu as pltpu
from jax.sharding import PartitionSpec as P

HD = 128
DRAFT = 16
STRIDE = 3
PIECES = 2
BATCH = 8
FAR = -1e30
FLOOR = -1e29
MESH = pl.DeviceIdType.MESH
F32 = jnp.float32
BF16 = jnp.bfloat16


def iota(shape, dim):
    return lax.broadcasted_iota(jnp.int32, shape, dim)


class Tree:
    def __init__(self, n, stride):
        self.stride = stride
        self.parent = {}
        for side, most in ((1, n // 2), (-1, n // 2 - 1)):
            for d in range(1, most + 1):
                over = d % stride
                up = d - over + stride
                if over == 0:
                    self.parent[side * d] = side * (d - stride)
                elif stride - over < over and up <= most:
                    self.parent[side * d] = side * up
                else:
                    self.parent[side * d] = side * (d - over)
        self.kids = {x: [] for x in [0, *self.parent]}
        for x, p in self.parent.items():
            self.kids[p].append(x)
        for x in self.kids:
            self.kids[x].sort(key=lambda y: (-len(self.kids[y]), -abs(self.hop(y)), y))
        self.order = sorted(self.parent, key=lambda x: (self.level(x), abs(x), x))
        self.index = {x: i for i, x in enumerate(sorted(self.parent))}
        self.stage = {x: i for i, x in enumerate(x for x in self.order if self.kids[x])}

    def hop(self, x):
        return x - self.parent[x]

    def level(self, x):
        if abs(x) % self.stride == 0:
            return 2 * abs(x) // self.stride
        return self.level(self.parent[x]) + 3


def tail_of(peak, total):
    high = total.astype(BF16).astype(F32)
    low = total - high
    row = iota((16, peak.shape[1]), 0)
    tile = jnp.where(row == 0, peak, jnp.where(row == 1, high, jnp.where(row == 2, low, 0.0)))
    return tile.astype(BF16)


def merged_state(states):
    peak = functools.reduce(jnp.maximum, [s[1] for s in states])
    numerator, denominator = 0.0, 0.0
    for num, own_peak, den in states:
        factor = jnp.exp(own_peak - peak)
        numerator = numerator + num * factor
        denominator = denominator + den * factor
    return numerator, peak, denominator


def read_state(ref):
    num = ref[pl.ds(0, HD), :].astype(F32)
    tail = ref[pl.ds(HD, 16), :].astype(F32)
    return num, tail[0:1], tail[1:2] + tail[2:3]


def write_state(ref, partial):
    num, peak, den = partial
    ref[pl.ds(0, HD), :] = num.astype(BF16)
    ref[pl.ds(HD, 16), :] = tail_of(peak, den)


def partial_softmax(scores):
    peak = jnp.maximum(jnp.max(scores, axis=0, keepdims=True), FLOOR)
    peak = peak.astype(BF16).astype(F32)
    weights = jnp.exp(scores - peak)
    return weights, peak, jnp.sum(weights, axis=0, keepdims=True)


def kernel(
    nz,
    nh,
    tree,
    lengths,
    queries,
    fresh_k,
    fresh_v,
    gain,
    residual,
    key_hbm,
    value_hbm,
    wo_hbm,
    wg_hbm,
    wu_hbm,
    wd_hbm,
    out,
    keys,
    values,
    wo,
    w_in,
    w_down,
    load_sem,
    q_all,
    q_relay,
    kv_all,
    kv_send,
    kv_recv,
    bias,
    values_t,
    state,
    s_in,
    s_out,
    s_relay,
    s_kept,
    s_joined,
    attended,
    blocks,
    b_in,
    b_out,
    b_relay,
    b_kept,
    b_joined,
    lower,
    l_in,
    l_out,
    l_relay,
    l_kept,
    l_joined,
    resid,
    n_relay,
    scaled,
    squares,
    h_send,
    h_recv,
    acts,
    z_send,
    z_recv,
    y_send,
    y_recv,
    v_send,
    v_recv,
    pace,
    x_send,
    x_recv,
    e_send,
    e_recv,
):
    z = lax.axis_index("ffn")
    h = lax.axis_index("hidden")
    rows, columns = queries.shape
    seqs, block = keys.shape[0], keys.shape[1]
    kv_heads = keys.shape[2] // HD
    share = nz // kv_heads
    lanes = rows * columns // HD
    per = nz // nh
    rz, width = residual.shape
    inner = wg_hbm.shape[0]
    half = w_in.shape[0] // 2
    batches = nz // BATCH
    group = BATCH // nh

    def at_z(i):
        return lax.rem(i + nz, nz)

    def at_h(i):
        return lax.rem(i + nh, nh)

    loads = [
        pltpu.make_async_copy(src, dst, load_sem.at[i])
        for i, (src, dst) in enumerate(
            (
                (key_hbm, keys),
                (value_hbm, values),
                (wo_hbm, wo),
                (wg_hbm, w_in.at[pl.ds(0, inner)]),
                (wu_hbm, w_in.at[pl.ds(half, inner)]),
                (wd_hbm, w_down.at[pl.ds(0, inner)]),
            )
        )
    ]
    for load in loads:
        load.start()

    barrier = pltpu.get_barrier_semaphore()
    reach = max(share - 1, STRIDE)
    around = [d for d in range(-reach, reach + 1) if d != 0]
    for d in around:
        pl.semaphore_signal(barrier, inc=1, device_id={"ffn": at_z(z + d)}, device_id_type=MESH)
    for d in range(1, nh):
        pl.semaphore_signal(barrier, inc=1, device_id={"hidden": at_h(h + d)}, device_id_type=MESH)
    partner = h + 1 - 2 * (h % 2)
    across = sorted({side * tree.hop(x) for x in tree.order for side in (1, -1)})
    for d in across:
        pl.semaphore_signal(
            barrier, inc=1, device_id={"ffn": at_z(z + d), "hidden": partner}, device_id_type=MESH
        )

    row, lane = iota((rows, HD), 0), iota((rows, HD), 1)
    position = functools.reduce(
        jnp.add, [jnp.where(row // DRAFT == i, lengths[i], 0) for i in range(seqs)]
    )
    position = position + row % DRAFT
    steps = (lane % (HD // 2)).astype(F32)
    angle = position.astype(F32) * jnp.exp(steps * (-2.0 * math.log(500000.0) / HD))
    cosine = jnp.cos(angle)
    sine = jnp.sin(angle)
    sine = jnp.where(lane < HD // 2, -sine, sine)

    def rotate(x):
        return (x * cosine + pltpu.roll(x, HD // 2, 1) * sine).astype(BF16)

    for i in range(columns // HD):
        part = queries[:, pl.ds(i * HD, HD)].astype(F32)
        q_all[z, pl.ds(i * rows, rows), :] = rotate(part)

    shape = (seqs * block, lanes)
    row, lane = iota(shape, 0), iota(shape, 1)
    cached_seq, lane_seq = row // block, (lane % rows) // DRAFT
    length = functools.reduce(
        jnp.add, [jnp.where(cached_seq == i, lengths[i], 0) for i in range(seqs)]
    )
    usable = jnp.logical_and(cached_seq == lane_seq, z * block + row % block < length)
    bias[...] = jnp.where(usable, 0.0, FAR)
    for i in (0, 1):
        kv_all[i, share - 1] = (fresh_k, fresh_v)[i][...]
    pl.semaphore_wait(barrier, len(around) + nh - 1 + len(across))

    forwards = h % 2 == 1

    def remote(src, dst, send, recv, hop, across=False):
        device = {"ffn": at_z(z + hop)}
        if across:
            device["hidden"] = partner
        return pltpu.make_async_remote_copy(
            src_ref=src,
            dst_ref=dst,
            send_sem=send,
            recv_sem=recv,
            device_id=device,
            device_id_type=MESH,
        )

    def gather_tools(buf, relay, which, cut):
        def first_copy(x, j):
            slot = at_z(z - tree.parent[x])
            ref, i = cut(buf.at[slot], j), tree.index[x]
            return remote(ref, ref, z_send.at[which, i, j], z_recv.at[which, i, j], tree.hop(x))

        def second_copy(x, j):
            p, i = tree.parent[x], tree.index[x]
            slot = at_z(z - p)
            src = cut(buf.at[slot] if p == 0 else relay.at[tree.stage[p]], j)
            if x in tree.stage:
                dst, recv = cut(relay.at[tree.stage[x]], j), y_recv.at[which, i, j]
            else:
                dst, recv = cut(buf.at[slot], j), z_recv.at[which, i, j]
            across = (p == 0) == (x in tree.stage)
            return remote(src, dst, y_send.at[which, i, j], recv, tree.hop(x), across)

        def handed(x, j):
            dst = cut(buf.at[at_z(z - x)], j)
            i = tree.index[x]
            return remote(
                cut(relay.at[tree.stage[x]], j), dst, v_send.at[which, tree.stage[x], j],
                z_recv.at[which, i, j], 0, True,
            )

        def first():
            for j in range(PIECES):
                for x in tree.kids[0]:

                    @pl.when(forwards)
                    def _():
                        first_copy(x, j).start()

                    @pl.when(jnp.logical_not(forwards))
                    def _():
                        second_copy(x, j).start()

        def rest(size, process):
            missing = [
                {-d % nz for side in (0, 1) for d in span_of(t, size, side)}
                for t in range(nz // (2 * size))
            ]
            missing[0].discard(0)
            for x in tree.order:
                for j in range(PIECES):
                    i = tree.index[x]
                    here = cut(buf.at[at_z(z - x)], j)
                    remote(here, here, z_send.at[which, i, j], z_recv.at[which, i, j], -1).wait_recv()
                    if x in tree.stage:

                        @pl.when(forwards)
                        def _():
                            for y in tree.kids[x]:
                                first_copy(y, j).start()
                            passing = cut(relay.at[tree.stage[x]], j)
                            remote(
                                passing, passing, y_send.at[which, i, j], y_recv.at[which, i, j], -1
                            ).wait_recv()
                            for y in tree.kids[x]:
                                second_copy(y, j).start()
                            handed(x, j).start()

                for t, labels in enumerate(missing):
                    if x % nz in labels:
                        labels.discard(x % nz)
                        if not labels:
                            process(t)

        def drain():
            @pl.when(forwards)
            def _():
                for j in range(PIECES):
                    for x in tree.order:
                        first_copy(x, j).wait_send()
                        if tree.parent[x] != 0:
                            second_copy(x, j).wait_send()
                        if x in tree.stage:
                            handed(x, j).wait_send()

            @pl.when(jnp.logical_not(forwards))
            def _():
                for j in range(PIECES):
                    for x in tree.kids[0]:
                        second_copy(x, j).wait_send()

        return first, rest, drain

    def span_of(t, size, side):
        if side == 0:
            return range(size * t, size * (t + 1))
        return range(-size * (t + 1), -size * t)

    def offset_in(t, size, i):
        return jnp.where(i < size, size * t + i, -size * (t + 1) + i - size)

    def scatter_tools(blk, incoming, staged, relay, relay_own, relay_out, which, pieces, cut, read, join, write):
        def first_copy(x, j):
            i = tree.index[x]
            own = blk.at[at_z(z - x)] if x not in tree.stage else staged.at[tree.stage[x]]
            return remote(
                cut(own, j), cut(incoming.at[i], j), z_send.at[which, i, j], z_recv.at[which, i, j],
                -tree.hop(x),
            )

        def second_copy(x, j):
            i, leaf = tree.index[x], x not in tree.stage
            src = cut(blk.at[at_z(z - x)] if leaf else relay_out.at[tree.stage[x]], j)
            if tree.parent[x] == 0:
                dst, recv = cut(incoming.at[i], j), z_recv.at[which, i, j]
            else:
                dst, recv = cut(relay.at[i], j), y_recv.at[which, i, j]
            across = leaf != (tree.parent[x] == 0)
            return remote(src, dst, y_send.at[which, i, j], recv, -tree.hop(x), across)

        def handed(x, j):
            k = tree.stage[x]
            return remote(
                cut(blk.at[at_z(z - x)], j), cut(relay_own.at[k], j), v_send.at[which, k, j],
                v_recv.at[which, k, j], 0, True,
            )

        def taken(kids, j, box, sems):
            terms = []
            for y in kids:
                i = tree.index[y]
                here = cut(box.at[i], j)
                remote(here, here, z_send.at[which, i, j], sems.at[which, i, j], -1).wait_recv()
                terms.append(read(here))
            return terms

        def split(x):
            kids = tree.kids[x]
            return [y for y in kids if not tree.kids[y]], [y for y in kids if tree.kids[y]]

        def early(x, j, more=()):
            own = [read(cut(blk.at[at_z(z - x)], j)), *more]
            return join([*own, *taken(split(x)[0], j, incoming, z_recv)])

        def late(x, j, value):
            return join([value, *taken(split(x)[1], j, incoming, z_recv)])

        def second_early(x, j):
            k = tree.stage[x]
            here = cut(relay_own.at[k], j)
            remote(here, here, v_send.at[which, k, j], v_recv.at[which, k, j], 0, True).wait_recv()
            return join([read(here), *taken(split(x)[0], j, relay, y_recv)])

        def second_late(x, j, value):
            return join([value, *taken(split(x)[1], j, relay, y_recv)])

        def run(before=lambda distance: None, more=lambda j: ()):
            order = list(reversed(tree.order))
            while order:
                both = [order.pop(0)]
                if order and order[0] == -both[0]:
                    both.append(order.pop(0))
                before(abs(both[0]))
                nodes = [x for x in both if x in tree.stage]
                leaves = [x for x in both if x not in tree.stage]

                @pl.when(forwards)
                def _():
                    for x in leaves:
                        for j in range(pieces):
                            first_copy(x, j).start()
                    ahead = {(x, j): early(x, j) for x in nodes for j in range(pieces)}
                    for j in range(pieces):
                        for x in nodes:
                            write(cut(staged.at[tree.stage[x]], j), late(x, j, ahead[x, j]))
                            first_copy(x, j).start()
                    ahead = {(x, j): second_early(x, j) for x in nodes for j in range(pieces)}
                    for j in range(pieces):
                        for x in nodes:
                            write(cut(relay_out.at[tree.stage[x]], j), second_late(x, j, ahead[x, j]))
                            second_copy(x, j).start()
                    if nodes:
                        pl.semaphore_signal(
                            pace.at[which], inc=1, device_id={"hidden": partner}, device_id_type=MESH
                        )

                @pl.when(jnp.logical_not(forwards))
                def _():
                    for j in range(pieces):
                        for x in leaves:
                            second_copy(x, j).start()
                        for x in nodes:
                            handed(x, j).start()
                    if nodes:
                        pl.semaphore_wait(pace.at[which], 1)

            before(0)
            ahead = [early(0, j, more(j)) for j in range(pieces)]
            return [late(0, j, ahead[j]) for j in range(pieces)]

        def drain():
            @pl.when(forwards)
            def _():
                for j in range(pieces):
                    for x in tree.order:
                        first_copy(x, j).wait_send()
                        if x in tree.stage:
                            second_copy(x, j).wait_send()

            @pl.when(jnp.logical_not(forwards))
            def _():
                for j in range(pieces):
                    for x in tree.order:
                        if x in tree.stage:
                            handed(x, j).wait_send()
                        else:
                            second_copy(x, j).wait_send()

        return run, drain

    def idle(steps):
        pending = list(steps)

        def before(distance):
            while pending and distance <= pending[0][0]:
                pending.pop(0)[1]()

        return before

    def peer_copy(send, recv, d, src, dst):
        return pltpu.make_async_remote_copy(
            src_ref=src,
            dst_ref=dst,
            send_sem=send.at[d],
            recv_sem=recv.at[d],
            device_id={"hidden": at_h(h + d)},
            device_id_type=MESH,
        )

    def whole(ref, j):
        return ref

    def cut_rows(ref, j):
        size = lanes // PIECES
        return ref.at[pl.ds(j * size, size)]

    def columns_of(j):
        size = width // PIECES
        return pl.ds(j * size, size)

    def cut_columns(ref, j):
        return ref.at[:, columns_of(j)]

    q_first, q_rest, q_drain = gather_tools(q_all, q_relay, 0, cut_rows)
    q_first()
    near = [d for d in range(-(share - 1), share) if d != 0]

    def kv_copy(i, d):
        return pltpu.make_async_remote_copy(
            src_ref=(fresh_k, fresh_v)[i],
            dst_ref=kv_all.at[i, share - 1 - d],
            send_sem=kv_send.at[i, d + share - 1],
            recv_sem=kv_recv.at[i, share - 1 - d],
            device_id={"ffn": at_z(z + d)},
            device_id_type=MESH,
        )

    for d in near:
        for i in (0, 1):
            kv_copy(i, d).start()
    scaling = 1.0 / math.sqrt(HD)
    loads[1].wait()

    @pl.loop(0, kv_heads)
    def _(k):
        head = values[:, :, pl.ds(pl.multiple_of(k * HD, HD), HD)].reshape(seqs * block, HD)
        values_t[k] = head.astype(F32).T.astype(BF16)

    loads[0].wait()

    def attend(t):
        for i in range(4):
            slot = at_z(z + offset_in(t, 2, i))
            k = slot // share
            head = keys[:, :, pl.ds(pl.multiple_of(k * HD, HD), HD)].reshape(seqs * block, HD)
            scores = lax.dot_general(
                head, q_all[slot], (((1,), (1,)), ((), ())), preferred_element_type=F32
            )
            weights, peak, den = partial_softmax(scores * scaling + bias[...])
            num = jnp.dot(values_t[k], weights.astype(BF16), preferred_element_type=F32)
            write_state(state.at[slot], (num, peak, den))

    q_rest(2, attend)

    for i in (0, 1):
        for d in near:
            kv_copy(i, d).wait_recv()
    first_of_head = share - 1 - z % share
    fresh = [
        jnp.concatenate([kv_all[i, first_of_head + j] for j in range(share)], axis=0)
        for i in (0, 1)
    ]
    draft_scores = lax.dot_general(
        rotate(fresh[0].astype(F32).T),
        q_all[z],
        (((1,), (1,)), ((), ())),
        preferred_element_type=F32,
    )
    row, lane = iota((rows, lanes), 0), iota((rows, lanes), 1)
    causal = jnp.logical_and(
        row // DRAFT == (lane % rows) // DRAFT, row % DRAFT <= lane % DRAFT
    )

    weights, peak, den = partial_softmax(jnp.where(causal, draft_scores * scaling, FAR))
    num = jnp.dot(fresh[1], weights.astype(BF16), preferred_element_type=F32)
    s_run, s_drain = scatter_tools(
        state, s_in, s_out, s_relay, s_kept, s_joined, 1, 1, whole, read_state, merged_state, write_state
    )
    num, _, den = s_run(idle([(9, q_drain)]), lambda j: [(num, peak, den)])[0]
    attended[h] = (num / den).T.astype(BF16)

    for d in range(1, nh):
        peer_copy(x_send, x_recv, d, attended.at[h], attended.at[h]).start()
    loads[2].wait()

    def project(c):
        d = at_h(h - c)

        @pl.when(d != 0)
        def _():
            peer_copy(x_send, x_recv, d, attended.at[c], attended.at[c]).wait_recv()

        pair = attended[c]
        both = jnp.concatenate([pair[:rows], pair[rows:]], axis=1)
        product = jnp.dot(both, wo[...], preferred_element_type=F32).astype(BF16)
        blocks[pl.ds(c * per, per)] = product.reshape(per, rz, width)

    done = set()
    center = z // per

    def project_for(distance):
        for j in range(nh // 2, distance // per - 1, -1):
            if j not in done:
                done.add(j)
                project(at_h(center + j))
                if 0 < j < nh // 2:
                    project(at_h(center - j))

    project_for(nz // 2 - 1)

    def widened(ref):
        return ref[...].astype(F32)

    def total(terms):
        return functools.reduce(jnp.add, terms)

    def rounded_to(ref, value):
        ref[...] = value.astype(BF16)

    def sum_tools(buffers, which):
        return scatter_tools(*buffers, which, PIECES, cut_columns, widened, total, rounded_to)

    p_run, p_drain = sum_tools((blocks, b_in, b_out, b_relay, b_kept, b_joined), 2)
    free = idle([(6, s_drain)])

    def between(distance):
        project_for(distance)
        free(distance)

    last = p_run(between, lambda j: [residual[:, columns_of(j)].astype(F32)])
    for j in range(PIECES):
        resid[z, :, columns_of(j)] = last[j].astype(BF16)

    n_first, n_rest, n_drain = gather_tools(resid, n_relay, 3, cut_columns)
    n_first()
    for load in loads[3:]:
        load.wait()
    gap = half - inner
    w_in[pl.ds(inner, gap), :] = jnp.zeros((gap, width), BF16)
    w_in[pl.ds(half + inner, gap), :] = jnp.zeros((gap, width), BF16)
    w_down[pl.ds(inner, gap), :] = jnp.zeros((gap, width), BF16)

    def inner_sums(t):
        @pl.loop(0, BATCH)
        def _(i):
            slot = at_z(z + offset_in(t, BATCH // 2, i))
            x = resid[slot].astype(F32)
            ssq = jnp.sum(x * x, axis=1, keepdims=True)
            squares[t, i] = jnp.broadcast_to(ssq, (rz, HD))
            for j in range(width // HD):
                cut = slice(j * HD, (j + 1) * HD)
                factor = gain[pl.ds(j, 1), :].astype(F32)
                scaled[t, i, :, pl.ds(j * HD, HD)] = (x[:, cut] * factor).astype(BF16)

        lhs = scaled[t].reshape(BATCH * rz, width)
        sums = lax.dot_general(
            lhs, w_in[...], (((1,), (1,)), ((), ())), preferred_element_type=F32
        )
        ssq = squares[t].reshape(BATCH * rz, HD)
        high = ssq.astype(BF16).astype(F32)
        column = iota((BATCH * rz, HD), 1)
        extra = jnp.where(column == HD - 2, high, jnp.where(column == HD - 1, ssq - high, 0.0))
        for at, size, piece in (
            (0, half - HD, sums[:, : half - HD]),
            (half - HD, HD, sums[:, half - HD : half] + extra),
            (half, half, sums[:, half:]),
        ):
            h_send[t, :, :, pl.ds(at, size)] = piece.astype(BF16).reshape(nh, group * rz, size)
        h_recv[t, h] = h_send[t, h]
        for d in range(1, nh):
            gate_copy(t, d).start()

    def gate_copy(t, d):
        return peer_copy(
            e_send.at[0, t], e_recv.at[0, t], d, h_send.at[t, at_h(h + d)], h_recv.at[t, h]
        )

    def activate(t):
        for d in range(1, nh):
            peer = at_h(h - d)
            peer_copy(
                e_send.at[0, t], e_recv.at[0, t], d, h_recv.at[t, peer], h_recv.at[t, peer]
            ).wait_recv()
        sums = total([widened(h_recv.at[t, i]) for i in range(nh)])
        edge = sums[:, half - HD : half]
        lane = iota(edge.shape, 1)
        ssq = jnp.sum(jnp.where(lane >= HD - 2, edge, 0.0), axis=1, keepdims=True)
        factor = lax.rsqrt(ssq / (nh * width) + 1e-05)
        gate, up = sums[:, :half] * factor, sums[:, half:] * factor
        gate = jnp.where(iota(gate.shape, 1) < inner, gate, 0.0)
        acts[t, h] = (gate / (1.0 + jnp.exp(-gate)) * up).astype(BF16)
        for d in range(1, nh):
            act_copy(t, d).start()

    def act_copy(t, d):
        return peer_copy(e_send.at[1, t], e_recv.at[1, t], d, acts.at[t, h], acts.at[t, h])

    def descend(t):
        for d in range(1, nh):
            peer = at_h(h - d)
            peer_copy(
                e_send.at[1, t], e_recv.at[1, t], d, acts.at[t, peer], acts.at[t, peer]
            ).wait_recv()
        lhs = acts[t].reshape(BATCH * rz, half)
        product = jnp.dot(lhs, w_down[...], preferred_element_type=F32).astype(BF16)
        product = product.reshape(BATCH, rz, width)
        for i in range(BATCH):
            lower[at_z(z + offset_in(t, BATCH // 2, i))] = product[i]

    def stages(t):
        inner_sums(t)
        if t >= 1:
            activate(t - 1)
        if t >= 2:
            descend(t - 2)

    n_rest(BATCH // 2, stages)
    if batches >= 2:
        descend(batches - 2)
    activate(batches - 1)
    descend(batches - 1)
    d_run, d_drain = sum_tools((lower, l_in, l_out, l_relay, l_kept, l_joined), 4)

    def rest_drain():
        for d in near:
            for i in (0, 1):
                kv_copy(i, d).wait_send()
        for d in range(1, nh):
            peer_copy(x_send, x_recv, d, attended.at[h], attended.at[h]).wait_send()
            for t in range(batches):
                gate_copy(t, d).wait_send()
                act_copy(t, d).wait_send()

    last = d_run(
        idle([(9, p_drain), (6, n_drain), (3, rest_drain)]),
        lambda j: [resid[z, :, columns_of(j)].astype(F32)],
    )
    for j in range(PIECES):
        out[:, columns_of(j)] = last[j].astype(BF16)

    d_drain()


def shards(
    residual_in,
    queries,
    new_keys,
    new_values,
    key_cache,
    value_cache,
    cache_lengths,
    norm_gain,
    out_weight,
    gate_weight,
    up_weight,
    down_weight,
):
    nz, nh = lax.axis_size("ffn"), lax.axis_size("hidden")
    rows, columns = queries.shape
    seqs, block, kv_width = key_cache.shape
    kv_heads = kv_width // HD
    share = nz // kv_heads
    rz, width = residual_in.shape
    inner = gate_weight.shape[1]
    half = -(-(inner + 2) // HD) * HD
    lanes = columns // HD * rows
    batches = nz // BATCH
    tree = Tree(nz, STRIDE)
    inside = len(tree.stage)
    vmem = pl.BlockSpec(memory_space=pltpu.VMEM)
    anywhere = pl.BlockSpec(memory_space=pl.ANY)
    dma = pltpu.SemaphoreType.DMA
    extent = HD + 16

    def scatter_buffers(shape):
        return [
            pltpu.VMEM((nz, *shape), BF16),
            pltpu.VMEM((nz - 1, *shape), BF16),
            pltpu.VMEM((inside, *shape), BF16),
            pltpu.VMEM((nz - 1, *shape), BF16),
            pltpu.VMEM((inside, *shape), BF16),
            pltpu.VMEM((inside, *shape), BF16),
        ]

    state_buffers = scatter_buffers((extent, lanes))
    sum_buffers = scatter_buffers((rz, width))
    scratch = [
        pltpu.VMEM(key_cache.shape, BF16),
        pltpu.VMEM(value_cache.shape, BF16),
        pltpu.VMEM(out_weight.shape, BF16),
        pltpu.VMEM((2 * half, width), BF16),
        pltpu.VMEM((half, width), BF16),
        dma((6,)),
        pltpu.VMEM((nz, lanes, HD), BF16),
        pltpu.VMEM((inside, lanes, HD), BF16),
        pltpu.VMEM((2, 2 * share - 1, HD // share, rows), BF16),
        dma((2, 2 * share - 1)),
        dma((2, 2 * share - 1)),
        pltpu.VMEM((seqs * block, lanes), F32),
        pltpu.VMEM((kv_heads, HD, seqs * block), BF16),
        *state_buffers,
        pltpu.VMEM((nh, lanes, HD), BF16),
        *sum_buffers,
        *sum_buffers,
        pltpu.VMEM((nz, rz, width), BF16),
        pltpu.VMEM((inside, rz, width), BF16),
        pltpu.VMEM((batches, BATCH, rz, width), BF16),
        pltpu.VMEM((batches, BATCH, rz, HD), F32),
        pltpu.VMEM((batches, nh, BATCH // nh * rz, 2 * half), BF16),
        pltpu.VMEM((batches, nh, BATCH // nh * rz, 2 * half), BF16),
        pltpu.VMEM((batches, nh, BATCH // nh * rz, half), BF16),
        dma((5, nz - 1, PIECES)),
        dma((5, nz - 1, PIECES)),
        dma((5, nz - 1, PIECES)),
        dma((5, nz - 1, PIECES)),
        dma((5, inside, PIECES)),
        dma((5, inside, PIECES)),
        pltpu.SemaphoreType.REGULAR((5,)),
        dma((nh,)),
        dma((nh,)),
        dma((2, batches, nh)),
        dma((2, batches, nh)),
    ]
    return pl.pallas_call(
        functools.partial(kernel, nz, nh, tree),
        out_shape=jax.ShapeDtypeStruct(residual_in.shape, BF16),
        in_specs=[pl.BlockSpec(memory_space=pltpu.SMEM)] + [vmem] * 5 + [anywhere] * 6,
        out_specs=vmem,
        scratch_shapes=scratch,
        compiler_params=pltpu.CompilerParams(
            collective_id=0, has_side_effects=True, vmem_limit_bytes=60 * 1024 * 1024
        ),
        name="block_step",
    )(
        cache_lengths,
        queries,
        new_keys.T,
        new_values.T,
        norm_gain.reshape(-1, HD),
        residual_in,
        key_cache,
        value_cache,
        out_weight,
        gate_weight.T,
        up_weight.T,
        down_weight,
    )


def solution(mesh):
    in_specs = (
        P(("groups", "ffn"), "hidden"),
        P(("groups", "hidden"), "ffn"),
        P(("groups", "hidden"), "ffn"),
        P(("groups", "hidden"), "ffn"),
        P(("groups", "hidden"), "ffn", None),
        P(("groups", "hidden"), "ffn", None),
        P(("groups", "hidden")),
        P("hidden"),
        P("ffn", "hidden"),
        P("hidden", "ffn"),
        P("hidden", "ffn"),
        P("ffn", "hidden"),
    )
    out_specs = P(("groups", "ffn"), "hidden")
    return jax.shard_map(shards, mesh=mesh, in_specs=in_specs, out_specs=out_specs, check_vma=False)
```

```python
import functools
import math

import jax
import jax.numpy as jnp
from jax import lax
from jax.experimental import pallas as pl
from jax.experimental.pallas import tpu as pltpu
from jax.sharding import PartitionSpec as P

HD = 128
DRAFT = 16
STRIDE = 3
PIECES = 2
BATCH = 8
FAR = -1e30
FLOOR = -1e29
MESH = pl.DeviceIdType.MESH
F32 = jnp.float32
BF16 = jnp.bfloat16


def iota(shape, dim):
    return lax.broadcasted_iota(jnp.int32, shape, dim)


class Tree:
    def __init__(self, n, stride):
        self.stride = stride
        self.parent = {}
        for side, most in ((1, n // 2), (-1, n // 2 - 1)):
            for d in range(1, most + 1):
                over = d % stride
                up = d - over + stride
                if over == 0:
                    self.parent[side * d] = side * (d - stride)
                elif stride - over < over and up <= most:
                    self.parent[side * d] = side * up
                else:
                    self.parent[side * d] = side * (d - over)
        self.kids = {x: [] for x in [0, *self.parent]}
        for x, p in self.parent.items():
            self.kids[p].append(x)
        for x in self.kids:
            self.kids[x].sort(key=lambda y: (-len(self.kids[y]), -abs(self.hop(y)), y))
        self.order = sorted(self.parent, key=lambda x: (self.level(x), abs(x), x))
        self.index = {x: i for i, x in enumerate(sorted(self.parent))}
        self.stage = {x: i for i, x in enumerate(x for x in self.order if self.kids[x])}

    def hop(self, x):
        return x - self.parent[x]

    def level(self, x):
        if abs(x) % self.stride == 0:
            return 2 * abs(x) // self.stride
        return self.level(self.parent[x]) + 3


def tail_of(peak, total):
    high = total.astype(BF16).astype(F32)
    low = total - high
    row = iota((16, peak.shape[1]), 0)
    tile = jnp.where(row == 0, peak, jnp.where(row == 1, high, jnp.where(row == 2, low, 0.0)))
    return tile.astype(BF16)


def merged_state(states):
    peak = functools.reduce(jnp.maximum, [s[1] for s in states])
    numerator, denominator = 0.0, 0.0
    for num, own_peak, den in states:
        factor = jnp.exp(own_peak - peak)
        numerator = numerator + num * factor
        denominator = denominator + den * factor
    return numerator, peak, denominator


def read_state(ref):
    num = ref[pl.ds(0, HD), :].astype(F32)
    tail = ref[pl.ds(HD, 16), :].astype(F32)
    return num, tail[0:1], tail[1:2] + tail[2:3]


def write_state(ref, partial):
    num, peak, den = partial
    ref[pl.ds(0, HD), :] = num.astype(BF16)
    ref[pl.ds(HD, 16), :] = tail_of(peak, den)


def partial_softmax(scores):
    peak = jnp.maximum(jnp.max(scores, axis=0, keepdims=True), FLOOR)
    peak = peak.astype(BF16).astype(F32)
    weights = jnp.exp(scores - peak)
    return weights, peak, jnp.sum(weights, axis=0, keepdims=True)


def kernel(
    nz,
    nh,
    tree,
    lengths,
    queries,
    fresh_k,
    fresh_v,
    gain,
    residual,
    key_hbm,
    value_hbm,
    wo_hbm,
    wg_hbm,
    wu_hbm,
    wd_hbm,
    out,
    keys,
    values,
    wo,
    w_in,
    w_down,
    load_sem,
    q_all,
    q_relay,
    kv_all,
    kv_send,
    kv_recv,
    bias,
    values_t,
    state,
    s_in,
    s_out,
    s_relay,
    s_kept,
    s_joined,
    attended,
    blocks,
    b_in,
    b_out,
    b_relay,
    b_kept,
    b_joined,
    lower,
    l_in,
    l_out,
    l_relay,
    l_kept,
    l_joined,
    resid,
    n_relay,
    scaled,
    squares,
    h_send,
    h_recv,
    acts,
    z_send,
    z_recv,
    y_send,
    y_recv,
    v_send,
    v_recv,
    pace,
    x_send,
    x_recv,
    e_send,
    e_recv,
):
    z = lax.axis_index("ffn")
    h = lax.axis_index("hidden")
    rows, columns = queries.shape
    seqs, block = keys.shape[0], keys.shape[1]
    kv_heads = keys.shape[2] // HD
    share = nz // kv_heads
    lanes = rows * columns // HD
    per = nz // nh
    rz, width = residual.shape
    inner = wg_hbm.shape[0]
    half = w_in.shape[0] // 2
    batches = nz // BATCH
    group = BATCH // nh

    def at_z(i):
        return lax.rem(i + nz, nz)

    def at_h(i):
        return lax.rem(i + nh, nh)

    loads = [
        pltpu.make_async_copy(src, dst, load_sem.at[i])
        for i, (src, dst) in enumerate(
            (
                (key_hbm, keys),
                (value_hbm, values),
                (wo_hbm, wo),
                (wg_hbm, w_in.at[pl.ds(0, inner)]),
                (wu_hbm, w_in.at[pl.ds(half, inner)]),
                (wd_hbm, w_down.at[pl.ds(0, inner)]),
            )
        )
    ]
    for load in loads:
        load.start()

    barrier = pltpu.get_barrier_semaphore()
    reach = max(share - 1, STRIDE)
    around = [d for d in range(-reach, reach + 1) if d != 0]
    for d in around:
        pl.semaphore_signal(barrier, inc=1, device_id={"ffn": at_z(z + d)}, device_id_type=MESH)
    for d in range(1, nh):
        pl.semaphore_signal(barrier, inc=1, device_id={"hidden": at_h(h + d)}, device_id_type=MESH)
    partner = h + 1 - 2 * (h % 2)
    across = sorted({side * tree.hop(x) for x in tree.order for side in (1, -1)})
    for d in across:
        pl.semaphore_signal(
            barrier, inc=1, device_id={"ffn": at_z(z + d), "hidden": partner}, device_id_type=MESH
        )

    row, lane = iota((rows, HD), 0), iota((rows, HD), 1)
    position = functools.reduce(
        jnp.add, [jnp.where(row // DRAFT == i, lengths[i], 0) for i in range(seqs)]
    )
    position = position + row % DRAFT
    steps = (lane % (HD // 2)).astype(F32)
    angle = position.astype(F32) * jnp.exp(steps * (-2.0 * math.log(500000.0) / HD))
    cosine = jnp.cos(angle)
    sine = jnp.sin(angle)
    sine = jnp.where(lane < HD // 2, -sine, sine)

    def rotate(x):
        return (x * cosine + pltpu.roll(x, HD // 2, 1) * sine).astype(BF16)

    for i in range(columns // HD):
        part = queries[:, pl.ds(i * HD, HD)].astype(F32)
        q_all[z, pl.ds(i * rows, rows), :] = rotate(part)

    shape = (seqs * block, lanes)
    row, lane = iota(shape, 0), iota(shape, 1)
    cached_seq, lane_seq = row // block, (lane % rows) // DRAFT
    length = functools.reduce(
        jnp.add, [jnp.where(cached_seq == i, lengths[i], 0) for i in range(seqs)]
    )
    usable = jnp.logical_and(cached_seq == lane_seq, z * block + row % block < length)
    bias[...] = jnp.where(usable, 0.0, FAR)
    for i in (0, 1):
        kv_all[i, share - 1] = (fresh_k, fresh_v)[i][...]
    pl.semaphore_wait(barrier, len(around) + nh - 1 + len(across))

    forwards = h % 2 == 1

    def remote(src, dst, send, recv, hop, across=False):
        device = {"ffn": at_z(z + hop)}
        if across:
            device["hidden"] = partner
        return pltpu.make_async_remote_copy(
            src_ref=src,
            dst_ref=dst,
            send_sem=send,
            recv_sem=recv,
            device_id=device,
            device_id_type=MESH,
        )

    def gather_tools(buf, relay, which, cut):
        def first_copy(x, j):
            slot = at_z(z - tree.parent[x])
            ref, i = cut(buf.at[slot], j), tree.index[x]
            return remote(ref, ref, z_send.at[which, i, j], z_recv.at[which, i, j], tree.hop(x))

        def second_copy(x, j):
            p, i = tree.parent[x], tree.index[x]
            slot = at_z(z - p)
            src = cut(buf.at[slot] if p == 0 else relay.at[tree.stage[p]], j)
            if x in tree.stage:
                dst, recv = cut(relay.at[tree.stage[x]], j), y_recv.at[which, i, j]
            else:
                dst, recv = cut(buf.at[slot], j), z_recv.at[which, i, j]
            across = (p == 0) == (x in tree.stage)
            return remote(src, dst, y_send.at[which, i, j], recv, tree.hop(x), across)

        def handed(x, j):
            dst = cut(buf.at[at_z(z - x)], j)
            i = tree.index[x]
            return remote(
                cut(relay.at[tree.stage[x]], j), dst, v_send.at[which, tree.stage[x], j],
                z_recv.at[which, i, j], 0, True,
            )

        def first():
            for j in range(PIECES):
                for x in tree.kids[0]:

                    @pl.when(forwards)
                    def _():
                        first_copy(x, j).start()

                    @pl.when(jnp.logical_not(forwards))
                    def _():
                        second_copy(x, j).start()

        def rest(size, process):
            missing = [
                {-d % nz for side in (0, 1) for d in span_of(t, size, side)}
                for t in range(nz // (2 * size))
            ]
            missing[0].discard(0)
            for x in tree.order:
                for j in range(PIECES):
                    i = tree.index[x]
                    here = cut(buf.at[at_z(z - x)], j)
                    remote(here, here, z_send.at[which, i, j], z_recv.at[which, i, j], -1).wait_recv()
                    if x in tree.stage:

                        @pl.when(forwards)
                        def _():
                            for y in tree.kids[x]:
                                first_copy(y, j).start()
                            passing = cut(relay.at[tree.stage[x]], j)
                            remote(
                                passing, passing, y_send.at[which, i, j], y_recv.at[which, i, j], -1
                            ).wait_recv()
                            for y in tree.kids[x]:
                                second_copy(y, j).start()
                            handed(x, j).start()

                for t, labels in enumerate(missing):
                    if x % nz in labels:
                        labels.discard(x % nz)
                        if not labels:
                            process(t)

        def drain():
            @pl.when(forwards)
            def _():
                for j in range(PIECES):
                    for x in tree.order:
                        first_copy(x, j).wait_send()
                        if tree.parent[x] != 0:
                            second_copy(x, j).wait_send()
                        if x in tree.stage:
                            handed(x, j).wait_send()

            @pl.when(jnp.logical_not(forwards))
            def _():
                for j in range(PIECES):
                    for x in tree.kids[0]:
                        second_copy(x, j).wait_send()

        return first, rest, drain

    def span_of(t, size, side):
        if side == 0:
            return range(size * t, size * (t + 1))
        return range(-size * (t + 1), -size * t)

    def offset_in(t, size, i):
        return jnp.where(i < size, size * t + i, -size * (t + 1) + i - size)

    def scatter_tools(blk, incoming, staged, relay, relay_own, relay_out, which, pieces, cut, read, join, write):
        def first_copy(x, j):
            i = tree.index[x]
            own = blk.at[at_z(z - x)] if x not in tree.stage else staged.at[tree.stage[x]]
            return remote(
                cut(own, j), cut(incoming.at[i], j), z_send.at[which, i, j], z_recv.at[which, i, j],
                -tree.hop(x),
            )

        def second_copy(x, j):
            i, leaf = tree.index[x], x not in tree.stage
            src = cut(blk.at[at_z(z - x)] if leaf else relay_out.at[tree.stage[x]], j)
            if tree.parent[x] == 0:
                dst, recv = cut(incoming.at[i], j), z_recv.at[which, i, j]
            else:
                dst, recv = cut(relay.at[i], j), y_recv.at[which, i, j]
            across = leaf != (tree.parent[x] == 0)
            return remote(src, dst, y_send.at[which, i, j], recv, -tree.hop(x), across)

        def handed(x, j):
            k = tree.stage[x]
            return remote(
                cut(blk.at[at_z(z - x)], j), cut(relay_own.at[k], j), v_send.at[which, k, j],
                v_recv.at[which, k, j], 0, True,
            )

        def taken(kids, j, box, sems):
            terms = []
            for y in kids:
                i = tree.index[y]
                here = cut(box.at[i], j)
                remote(here, here, z_send.at[which, i, j], sems.at[which, i, j], -1).wait_recv()
                terms.append(read(here))
            return terms

        def split(x):
            kids = tree.kids[x]
            return [y for y in kids if not tree.kids[y]], [y for y in kids if tree.kids[y]]

        def early(x, j, more=()):
            own = [read(cut(blk.at[at_z(z - x)], j)), *more]
            return join([*own, *taken(split(x)[0], j, incoming, z_recv)])

        def late(x, j, value):
            return join([value, *taken(split(x)[1], j, incoming, z_recv)])

        def second_early(x, j):
            k = tree.stage[x]
            here = cut(relay_own.at[k], j)
            remote(here, here, v_send.at[which, k, j], v_recv.at[which, k, j], 0, True).wait_recv()
            return join([read(here), *taken(split(x)[0], j, relay, y_recv)])

        def second_late(x, j, value):
            return join([value, *taken(split(x)[1], j, relay, y_recv)])

        def run(before=lambda distance: None, more=lambda j: ()):
            order = list(reversed(tree.order))
            while order:
                both = [order.pop(0)]
                if order and order[0] == -both[0]:
                    both.append(order.pop(0))
                before(abs(both[0]))
                nodes = [x for x in both if x in tree.stage]
                leaves = [x for x in both if x not in tree.stage]

                @pl.when(forwards)
                def _():
                    for x in leaves:
                        for j in range(pieces):
                            first_copy(x, j).start()
                    ahead = {(x, j): early(x, j) for x in nodes for j in range(pieces)}
                    for j in range(pieces):
                        for x in nodes:
                            write(cut(staged.at[tree.stage[x]], j), late(x, j, ahead[x, j]))
                            first_copy(x, j).start()
                    ahead = {(x, j): second_early(x, j) for x in nodes for j in range(pieces)}
                    for j in range(pieces):
                        for x in nodes:
                            write(cut(relay_out.at[tree.stage[x]], j), second_late(x, j, ahead[x, j]))
                            second_copy(x, j).start()
                    if nodes:
                        pl.semaphore_signal(
                            pace.at[which], inc=1, device_id={"hidden": partner}, device_id_type=MESH
                        )

                @pl.when(jnp.logical_not(forwards))
                def _():
                    for j in range(pieces):
                        for x in leaves:
                            second_copy(x, j).start()
                        for x in nodes:
                            handed(x, j).start()
                    if nodes:
                        pl.semaphore_wait(pace.at[which], 1)

            before(0)
            ahead = [early(0, j, more(j)) for j in range(pieces)]
            return [late(0, j, ahead[j]) for j in range(pieces)]

        def drain():
            @pl.when(forwards)
            def _():
                for j in range(pieces):
                    for x in tree.order:
                        first_copy(x, j).wait_send()
                        if x in tree.stage:
                            second_copy(x, j).wait_send()

            @pl.when(jnp.logical_not(forwards))
            def _():
                for j in range(pieces):
                    for x in tree.order:
                        if x in tree.stage:
                            handed(x, j).wait_send()
                        else:
                            second_copy(x, j).wait_send()

        return run, drain

    def idle(steps):
        pending = list(steps)

        def before(distance):
            while pending and distance <= pending[0][0]:
                pending.pop(0)[1]()

        return before

    def peer_copy(send, recv, d, src, dst):
        return pltpu.make_async_remote_copy(
            src_ref=src,
            dst_ref=dst,
            send_sem=send.at[d],
            recv_sem=recv.at[d],
            device_id={"hidden": at_h(h + d)},
            device_id_type=MESH,
        )

    def whole(ref, j):
        return ref

    def cut_rows(ref, j):
        size = lanes // PIECES
        return ref.at[pl.ds(j * size, size)]

    def columns_of(j):
        size = width // PIECES
        return pl.ds(j * size, size)

    def cut_columns(ref, j):
        return ref.at[:, columns_of(j)]

    q_first, q_rest, q_drain = gather_tools(q_all, q_relay, 0, cut_rows)
    q_first()
    near = [d for d in range(-(share - 1), share) if d != 0]

    def kv_copy(i, d):
        return pltpu.make_async_remote_copy(
            src_ref=(fresh_k, fresh_v)[i],
            dst_ref=kv_all.at[i, share - 1 - d],
            send_sem=kv_send.at[i, d + share - 1],
            recv_sem=kv_recv.at[i, share - 1 - d],
            device_id={"ffn": at_z(z + d)},
            device_id_type=MESH,
        )

    for d in near:
        for i in (0, 1):
            kv_copy(i, d).start()
    scaling = 1.0 / math.sqrt(HD)
    loads[1].wait()

    @pl.loop(0, kv_heads)
    def _(k):
        head = values[:, :, pl.ds(pl.multiple_of(k * HD, HD), HD)].reshape(seqs * block, HD)
        values_t[k] = head.astype(F32).T.astype(BF16)

    loads[0].wait()

    def attend(t):
        for i in range(4):
            slot = at_z(z + offset_in(t, 2, i))
            k = slot // share
            head = keys[:, :, pl.ds(pl.multiple_of(k * HD, HD), HD)].reshape(seqs * block, HD)
            scores = lax.dot_general(
                head, q_all[slot], (((1,), (1,)), ((), ())), preferred_element_type=F32
            )
            weights, peak, den = partial_softmax(scores * scaling + bias[...])
            num = jnp.dot(values_t[k], weights.astype(BF16), preferred_element_type=F32)
            write_state(state.at[slot], (num, peak, den))

    q_rest(2, attend)

    for i in (0, 1):
        for d in near:
            kv_copy(i, d).wait_recv()
    first_of_head = share - 1 - z % share
    fresh = [
        jnp.concatenate([kv_all[i, first_of_head + j] for j in range(share)], axis=0)
        for i in (0, 1)
    ]
    draft_scores = lax.dot_general(
        rotate(fresh[0].astype(F32).T),
        q_all[z],
        (((1,), (1,)), ((), ())),
        preferred_element_type=F32,
    )
    row, lane = iota((rows, lanes), 0), iota((rows, lanes), 1)
    causal = jnp.logical_and(
        row // DRAFT == (lane % rows) // DRAFT, row % DRAFT <= lane % DRAFT
    )

    weights, peak, den = partial_softmax(jnp.where(causal, draft_scores * scaling, FAR))
    num = jnp.dot(fresh[1], weights.astype(BF16), preferred_element_type=F32)
    s_run, s_drain = scatter_tools(
        state, s_in, s_out, s_relay, s_kept, s_joined, 1, 1, whole, read_state, merged_state, write_state
    )
    num, _, den = s_run(idle([(9, q_drain)]), lambda j: [(num, peak, den)])[0]
    attended[h] = (num / den).T.astype(BF16)

    for d in range(1, nh):
        peer_copy(x_send, x_recv, d, attended.at[h], attended.at[h]).start()
    loads[2].wait()

    def project(c):
        d = at_h(h - c)

        @pl.when(d != 0)
        def _():
            peer_copy(x_send, x_recv, d, attended.at[c], attended.at[c]).wait_recv()

        pair = attended[c]
        both = jnp.concatenate([pair[:rows], pair[rows:]], axis=1)
        product = jnp.dot(both, wo[...], preferred_element_type=F32).astype(BF16)
        blocks[pl.ds(c * per, per)] = product.reshape(per, rz, width)

    done = set()
    center = z // per

    def project_for(distance):
        for j in range(nh // 2, distance // per - 1, -1):
            if j not in done:
                done.add(j)
                project(at_h(center + j))
                if 0 < j < nh // 2:
                    project(at_h(center - j))

    project_for(nz // 2 - 1)

    def widened(ref):
        return ref[...].astype(F32)

    def total(terms):
        return functools.reduce(jnp.add, terms)

    def rounded_to(ref, value):
        ref[...] = value.astype(BF16)

    def sum_tools(buffers, which):
        return scatter_tools(*buffers, which, 1, whole, widened, total, rounded_to)

    p_run, p_drain = sum_tools((blocks, b_in, b_out, b_relay, b_kept, b_joined), 2)
    free = idle([(6, s_drain)])

    def between(distance):
        project_for(distance)
        free(distance)

    last = p_run(between, lambda j: [residual[...].astype(F32)])
    resid[z] = last[0].astype(BF16)

    n_first, n_rest, n_drain = gather_tools(resid, n_relay, 3, cut_columns)
    n_first()
    for load in loads[3:]:
        load.wait()
    gap = half - inner
    w_in[pl.ds(inner, gap), :] = jnp.zeros((gap, width), BF16)
    w_in[pl.ds(half + inner, gap), :] = jnp.zeros((gap, width), BF16)
    w_down[pl.ds(inner, gap), :] = jnp.zeros((gap, width), BF16)

    def inner_sums(t):
        @pl.loop(0, BATCH)
        def _(i):
            slot = at_z(z + offset_in(t, BATCH // 2, i))
            x = resid[slot].astype(F32)
            ssq = jnp.sum(x * x, axis=1, keepdims=True)
            squares[t, i] = jnp.broadcast_to(ssq, (rz, HD))
            for j in range(width // HD):
                cut = slice(j * HD, (j + 1) * HD)
                factor = gain[pl.ds(j, 1), :].astype(F32)
                scaled[t, i, :, pl.ds(j * HD, HD)] = (x[:, cut] * factor).astype(BF16)

        lhs = scaled[t].reshape(BATCH * rz, width)
        sums = lax.dot_general(
            lhs, w_in[...], (((1,), (1,)), ((), ())), preferred_element_type=F32
        )
        ssq = squares[t].reshape(BATCH * rz, HD)
        high = ssq.astype(BF16).astype(F32)
        column = iota((BATCH * rz, HD), 1)
        extra = jnp.where(column == HD - 2, high, jnp.where(column == HD - 1, ssq - high, 0.0))
        for at, size, piece in (
            (0, half - HD, sums[:, : half - HD]),
            (half - HD, HD, sums[:, half - HD : half] + extra),
            (half, half, sums[:, half:]),
        ):
            h_send[t, :, :, pl.ds(at, size)] = piece.astype(BF16).reshape(nh, group * rz, size)
        h_recv[t, h] = h_send[t, h]
        for d in range(1, nh):
            gate_copy(t, d).start()

    def gate_copy(t, d):
        return peer_copy(
            e_send.at[0, t], e_recv.at[0, t], d, h_send.at[t, at_h(h + d)], h_recv.at[t, h]
        )

    def activate(t):
        for d in range(1, nh):
            peer = at_h(h - d)
            peer_copy(
                e_send.at[0, t], e_recv.at[0, t], d, h_recv.at[t, peer], h_recv.at[t, peer]
            ).wait_recv()
        sums = total([widened(h_recv.at[t, i]) for i in range(nh)])
        edge = sums[:, half - HD : half]
        lane = iota(edge.shape, 1)
        ssq = jnp.sum(jnp.where(lane >= HD - 2, edge, 0.0), axis=1, keepdims=True)
        factor = lax.rsqrt(ssq / (nh * width) + 1e-05)
        gate, up = sums[:, :half] * factor, sums[:, half:] * factor
        gate = jnp.where(iota(gate.shape, 1) < inner, gate, 0.0)
        acts[t, h] = (gate / (1.0 + jnp.exp(-gate)) * up).astype(BF16)
        for d in range(1, nh):
            act_copy(t, d).start()

    def act_copy(t, d):
        return peer_copy(e_send.at[1, t], e_recv.at[1, t], d, acts.at[t, h], acts.at[t, h])

    def descend(t):
        for d in range(1, nh):
            peer = at_h(h - d)
            peer_copy(
                e_send.at[1, t], e_recv.at[1, t], d, acts.at[t, peer], acts.at[t, peer]
            ).wait_recv()
        lhs = acts[t].reshape(BATCH * rz, half)
        product = jnp.dot(lhs, w_down[...], preferred_element_type=F32).astype(BF16)
        product = product.reshape(BATCH, rz, width)
        for i in range(BATCH):
            lower[at_z(z + offset_in(t, BATCH // 2, i))] = product[i]

    def stages(t):
        inner_sums(t)
        if t >= 1:
            activate(t - 1)
        if t >= 2:
            descend(t - 2)

    n_rest(BATCH // 2, stages)
    if batches >= 2:
        descend(batches - 2)
    activate(batches - 1)
    descend(batches - 1)
    d_run, d_drain = sum_tools((lower, l_in, l_out, l_relay, l_kept, l_joined), 4)

    def rest_drain():
        for d in near:
            for i in (0, 1):
                kv_copy(i, d).wait_send()
        for d in range(1, nh):
            peer_copy(x_send, x_recv, d, attended.at[h], attended.at[h]).wait_send()
            for t in range(batches):
                gate_copy(t, d).wait_send()
                act_copy(t, d).wait_send()

    last = d_run(
        idle([(9, p_drain), (6, n_drain), (3, rest_drain)]),
        lambda j: [resid[z].astype(F32)],
    )
    out[...] = last[0].astype(BF16)

    d_drain()


def shards(
    residual_in,
    queries,
    new_keys,
    new_values,
    key_cache,
    value_cache,
    cache_lengths,
    norm_gain,
    out_weight,
    gate_weight,
    up_weight,
    down_weight,
):
    nz, nh = lax.axis_size("ffn"), lax.axis_size("hidden")
    rows, columns = queries.shape
    seqs, block, kv_width = key_cache.shape
    kv_heads = kv_width // HD
    share = nz // kv_heads
    rz, width = residual_in.shape
    inner = gate_weight.shape[1]
    half = -(-(inner + 2) // HD) * HD
    lanes = columns // HD * rows
    batches = nz // BATCH
    tree = Tree(nz, STRIDE)
    inside = len(tree.stage)
    vmem = pl.BlockSpec(memory_space=pltpu.VMEM)
    anywhere = pl.BlockSpec(memory_space=pl.ANY)
    dma = pltpu.SemaphoreType.DMA
    extent = HD + 16

    def scatter_buffers(shape):
        return [
            pltpu.VMEM((nz, *shape), BF16),
            pltpu.VMEM((nz - 1, *shape), BF16),
            pltpu.VMEM((inside, *shape), BF16),
            pltpu.VMEM((nz - 1, *shape), BF16),
            pltpu.VMEM((inside, *shape), BF16),
            pltpu.VMEM((inside, *shape), BF16),
        ]

    state_buffers = scatter_buffers((extent, lanes))
    sum_buffers = scatter_buffers((rz, width))
    scratch = [
        pltpu.VMEM(key_cache.shape, BF16),
        pltpu.VMEM(value_cache.shape, BF16),
        pltpu.VMEM(out_weight.shape, BF16),
        pltpu.VMEM((2 * half, width), BF16),
        pltpu.VMEM((half, width), BF16),
        dma((6,)),
        pltpu.VMEM((nz, lanes, HD), BF16),
        pltpu.VMEM((inside, lanes, HD), BF16),
        pltpu.VMEM((2, 2 * share - 1, HD // share, rows), BF16),
        dma((2, 2 * share - 1)),
        dma((2, 2 * share - 1)),
        pltpu.VMEM((seqs * block, lanes), F32),
        pltpu.VMEM((kv_heads, HD, seqs * block), BF16),
        *state_buffers,
        pltpu.VMEM((nh, lanes, HD), BF16),
        *sum_buffers,
        *sum_buffers,
        pltpu.VMEM((nz, rz, width), BF16),
        pltpu.VMEM((inside, rz, width), BF16),
        pltpu.VMEM((batches, BATCH, rz, width), BF16),
        pltpu.VMEM((batches, BATCH, rz, HD), F32),
        pltpu.VMEM((batches, nh, BATCH // nh * rz, 2 * half), BF16),
        pltpu.VMEM((batches, nh, BATCH // nh * rz, 2 * half), BF16),
        pltpu.VMEM((batches, nh, BATCH // nh * rz, half), BF16),
        dma((5, nz - 1, PIECES)),
        dma((5, nz - 1, PIECES)),
        dma((5, nz - 1, PIECES)),
        dma((5, nz - 1, PIECES)),
        dma((5, inside, PIECES)),
        dma((5, inside, PIECES)),
        pltpu.SemaphoreType.REGULAR((5,)),
        dma((nh,)),
        dma((nh,)),
        dma((2, batches, nh)),
        dma((2, batches, nh)),
    ]
    return pl.pallas_call(
        functools.partial(kernel, nz, nh, tree),
        out_shape=jax.ShapeDtypeStruct(residual_in.shape, BF16),
        in_specs=[pl.BlockSpec(memory_space=pltpu.SMEM)] + [vmem] * 5 + [anywhere] * 6,
        out_specs=vmem,
        scratch_shapes=scratch,
        compiler_params=pltpu.CompilerParams(
            collective_id=0, has_side_effects=True, vmem_limit_bytes=60 * 1024 * 1024
        ),
        name="block_step",
    )(
        cache_lengths,
        queries,
        new_keys.T,
        new_values.T,
        norm_gain.reshape(-1, HD),
        residual_in,
        key_cache,
        value_cache,
        out_weight,
        gate_weight.T,
        up_weight.T,
        down_weight,
    )


def solution(mesh):
    in_specs = (
        P(("groups", "ffn"), "hidden"),
        P(("groups", "hidden"), "ffn"),
        P(("groups", "hidden"), "ffn"),
        P(("groups", "hidden"), "ffn"),
        P(("groups", "hidden"), "ffn", None),
        P(("groups", "hidden"), "ffn", None),
        P(("groups", "hidden")),
        P("hidden"),
        P("ffn", "hidden"),
        P("hidden", "ffn"),
        P("hidden", "ffn"),
        P("ffn", "hidden"),
    )
    out_specs = P(("groups", "ffn"), "hidden")
    return jax.shard_map(shards, mesh=mesh, in_specs=in_specs, out_specs=out_specs, check_vma=False)
```
